32 devices in a mesh: groups: 2 (over y), dp: 4 (over z), rep: 4 (over x, core).
Axes of the slice: x: 2, y: 2, z: 4, core: 2. Of those that a mesh axis runs over, the one named last changes fastest.
Arguments:
- latent_store: bfloat16 [8, 48, 576, 128], P(('groups', 'dp'), 'rep'), parts along dimension 0, may hold values from -6 to 6
- page_rank: int32 [8, 48], P('groups', 'rep'), parts along dimension 0, may hold values from 0 to 3, as said below
- page_index: int32 [8, 48], P('groups', 'rep'), parts along dimension 0, may hold values from 0 to 11, as said below
- lengths: int32 [8, 1], P('groups'), parts along dimension 0, may hold values from 1536 to 6144, as said below
- queries: bfloat16 [16, 36864], P(('groups', 'dp')), parts along dimension 0, may hold values from -250 to 250
- new_latent: bfloat16 [16, 576], P(('groups', 'dp')), parts along dimension 0, may hold values from -4 to 4
- up_value: bfloat16 [64, 512, 128], P('dp'), may hold values from -0.25 to 0.25
- out_proj: bfloat16 [8192, 7168], P('dp', 'rep'), may hold values from -0.0625 to 0.0625
- residual: bfloat16 [16, 7168], P(('groups', 'dp'), 'rep'), parts along dimension 0, may hold values from -11 to 11
- norm_gain: float32 [7168], P('rep'), may hold values from 0.1 to 1.9
- w_gate: bfloat16 [7168, 12288], P('rep', 'dp'), may hold values from -0.0625 to 0.0625
- w_up: bfloat16 [7168, 12288], P('rep', 'dp'), may hold values from -0.0625 to 0.0625
- w_down: bfloat16 [12288, 7168], P('dp', 'rep'), may hold values from -0.0546875 to 0.0546875
Outputs:
- layer_out: bfloat16 [16, 7168], P(('groups', 'dp'), 'rep'), parts along dimension 0
The draws below stay inside these ranges and needn't reach their ends.
There are 2 independent parts, one for each index of `groups`. The reference program is written for one: setup_inputs(seed, part) draws one part's arguments, and reference() takes and returns one part's arrays. A program takes and returns all parts, laid end to end along the dimension named above; an argument that names none is the same for every part. Nothing has to cross between parts.
Inputs may be any that keep to these rules, and one draw needn't show every extreme that they name: page_rank[d, q] is the storage rank holding slot q of rank d, on its device with rep index q // 12; one storage device holds at most 3 slot of one rank, and some holds exactly 3. page_index[d, q] is the slot's page among the 12 pages of its storage device; over all ranks every page of every storage device is named by exactly one slot. `lengths`: some request has exactly 6144 tokens.
All inputs are finite; a program needn't handle non-finite values.
Results may differ from the reference program's by a relative error of at most 0.015.
Values may be sent and summed in bfloat16 or wider, within the bound.
A program may use at most 128 MiB of HBM per device.

```python
import jax
import jax.numpy as jnp
from jax import lax

D = 7168
HEADS = 64
CKV = 512
ROPE = 64
VDIM = 128
FF = 12288
PAGE = 128
STEPS = 2
REQ_DP = 1
PAGES = 48
LAT = 576
ROWS = 8
RANKS = 4
QSLOTS = 48
SLOT_DEV = 12


def permute_rows(source_key, count, length):
    row_keys = jax.random.split(source_key, count)
    return jax.vmap(lambda single: jax.random.permutation(single, length))(row_keys).astype(jnp.int32)


def page_tables(key):
    base_key = jax.random.fold_in(key, 11)
    columns = QSLOTS // SLOT_DEV
    key_list = jax.random.split(base_key, 5)
    outer_perm = permute_rows(key_list[0], columns, RANKS)
    inner_perm = permute_rows(key_list[1], columns, RANKS)
    offset_perm = permute_rows(key_list[2], columns, RANKS)
    virtual_slot = permute_rows(key_list[3], columns * RANKS, SLOT_DEV).reshape(columns, RANKS, SLOT_DEV)
    store_perm = permute_rows(key_list[4], columns * RANKS, SLOT_DEV).reshape(columns, RANKS * SLOT_DEV)
    offset_table = jnp.broadcast_to(offset_perm[:, None, :], (columns, RANKS, RANKS))
    offsets = jnp.take_along_axis(offset_table, virtual_slot % RANKS, axis=2)
    position = (inner_perm[:, :, None] + offsets) % RANKS
    outer_table = jnp.broadcast_to(outer_perm[:, None, :], (columns, RANKS, RANKS))
    source_rank = jnp.take_along_axis(outer_table, position, axis=2)
    store_table = jnp.broadcast_to(store_perm[:, None, :], (columns, RANKS, RANKS * SLOT_DEV))
    store_slot = jnp.take_along_axis(store_table, source_rank * SLOT_DEV + virtual_slot, axis=2)
    rank_table = source_rank.transpose(1, 0, 2).reshape(RANKS, QSLOTS).astype(jnp.int32)
    index_table = store_slot.transpose(1, 0, 2).reshape(RANKS, QSLOTS).astype(jnp.int32)
    return (rank_table, index_table)


def draw_page_rank(key, part):
    return page_tables(key)[0]


def draw_page_index(key, part):
    return page_tables(key)[1]


def draw_lengths(key, part):
    base_key = jax.random.fold_in(key, 31)
    first_key, second_key = jax.random.split(base_key)
    longest = PAGES * PAGE
    drawn = jax.random.randint(first_key, (RANKS * REQ_DP,), longest // 4, longest + 1, dtype=jnp.int32)
    marked = jax.random.randint(second_key, (), 0, RANKS * REQ_DP, dtype=jnp.int32)
    drawn = drawn.at[marked].set(longest)
    return drawn.reshape(RANKS, REQ_DP).astype(jnp.int32)


def latent_rows(key):
    base_key = jax.random.fold_in(key, 47)
    fresh = jax.random.truncated_normal(base_key, -4.0, 4.0, (ROWS // STEPS, STEPS, LAT), jnp.float32)
    return fresh


def draw_new_latent(key, part):
    return latent_rows(key).reshape(ROWS, LAT).astype(jnp.bfloat16)


def draw_queries(key, part):
    fresh = latent_rows(key)
    base_key = jax.random.fold_in(key, 53)
    first_key = jax.random.fold_in(base_key, 0)
    drawn = jax.random.truncated_normal(first_key, -4.0, 4.0, (ROWS // STEPS, STEPS, HEADS, LAT), jnp.float32)
    target = jnp.broadcast_to(fresh[:, :, None, CKV:], (ROWS // STEPS, STEPS, HEADS, ROPE))
    strength = jnp.full((ROWS // STEPS, STEPS, HEADS), 1.6, jnp.float32)
    drawn = drawn.at[..., CKV:].add(strength[..., None] * target)
    return drawn.reshape(ROWS, HEADS * LAT).astype(jnp.bfloat16)


def draw_residual(key, part):
    base_key = jax.random.fold_in(key, 61)
    first_key = jax.random.fold_in(base_key, 0)
    column = jnp.arange(D, dtype=jnp.float32) / D
    values = jax.random.truncated_normal(first_key, -5.0, 5.0, (ROWS, D), jnp.float32) * (1.0 + 0.8 * column)
    return values.astype(jnp.bfloat16)


def shard_levels(stream_key, shape, cuts, smallest, largest):
    gain, own = 1.0, jax.random.fold_in(stream_key, 6)
    for dim, shards_of in cuts:
        steps = jnp.exp(jax.random.uniform(jax.random.fold_in(own, dim), (shards_of,), jnp.float32, smallest / len(cuts), largest / len(cuts)))
        gain = gain * jnp.repeat(steps, shape[dim] // shards_of).reshape([-1 if axis == dim else 1 for axis in range(len(shape))])
    return gain


def gaussian(key, shape, width, bound, pieces=(), kind=jnp.bfloat16):
    result = jax.random.normal(key, shape, jnp.float32) * width
    if len(pieces) > 0:
        result = shard_levels(key, shape, pieces, -0.22, 0.18) * result
    return jnp.clip(result, min=-bound, max=bound).astype(kind)


def setup_inputs(seed: int = 0, part: int = 0) -> dict:
    seeds = jax.random.split(jax.random.key(seed), 14)
    part_splits = jax.random.split(jax.random.fold_in(seeds[13], part), 14)
    latent_store = gaussian(part_splits[0], (RANKS, QSLOTS, LAT, PAGE), 1.0, 6.0, ((0, 4), (1, 4)))
    page_rank = draw_page_rank(jax.random.fold_in(jax.random.fold_in(seeds[13], part), 71), part)
    page_index = draw_page_index(jax.random.fold_in(jax.random.fold_in(seeds[13], part), 71), part)
    lengths = draw_lengths(jax.random.fold_in(jax.random.fold_in(seeds[13], part), 71), part)
    queries = draw_queries(jax.random.fold_in(jax.random.fold_in(seeds[13], part), 71), part)
    new_latent = draw_new_latent(jax.random.fold_in(jax.random.fold_in(seeds[13], part), 71), part)
    up_value = gaussian(seeds[6], (HEADS, CKV, VDIM), CKV ** -0.5, 0.25, ((0, 4),))
    out_proj = gaussian(seeds[7], (HEADS * VDIM, D), (HEADS * VDIM) ** -0.5, 0.0625, ((0, 4), (1, 4)))
    residual = draw_residual(jax.random.fold_in(jax.random.fold_in(seeds[13], part), 71), part)
    norm_gain = jnp.clip(1.0 + 0.18 * jax.random.normal(seeds[9], (D,), jnp.float32), 0.1, 1.9)
    w_gate = gaussian(seeds[10], (D, FF), D ** -0.5, 0.0625, ((0, 4), (1, 4)))
    w_up = gaussian(seeds[11], (D, FF), D ** -0.5, 0.0625, ((0, 4), (1, 4)))
    w_down = gaussian(seeds[12], (FF, D), FF ** -0.5, 0.0546875, ((0, 4), (1, 4)))
    return {"latent_store": latent_store, "page_rank": page_rank, "page_index": page_index, "lengths": lengths, "queries": queries, "new_latent": new_latent, "up_value": up_value, "out_proj": out_proj, "residual": residual, "norm_gain": norm_gain, "w_gate": w_gate, "w_up": w_up, "w_down": w_down}


score_scale = 1.0 / 192.0 ** 0.5
epsilon = 1e-06
mask_value = -1e+30

def reference(latent_store, page_rank, page_index, lengths, queries, new_latent, up_value, out_proj, residual, norm_gain, w_gate, w_up, w_down):
    slot_ids = jnp.arange(QSLOTS, dtype=jnp.int32)
    store_base = (slot_ids // SLOT_DEV * SLOT_DEV).astype(jnp.int32)
    query_all = queries.reshape(RANKS, REQ_DP, STEPS, HEADS, LAT)
    fresh_all = new_latent.reshape(RANKS, REQ_DP, STEPS, LAT)

    def one_rank(inputs):
        rank_row, index_row, length_row, query_rank, fresh_rank = inputs
        pages = latent_store[rank_row.astype(jnp.int32), store_base + index_row.astype(jnp.int32)]
        context = pages.reshape(REQ_DP, PAGES, LAT, PAGE).transpose(0, 2, 1, 3).reshape(REQ_DP, LAT, PAGES * PAGE).astype(jnp.float32)
        query_f = query_rank.astype(jnp.float32)
        fresh_f = fresh_rank.astype(jnp.float32)
        context_scores = jnp.einsum('jshl,jlt->jsht', query_f, context) * score_scale
        positions = jnp.arange(PAGES * PAGE, dtype=jnp.int32)
        seen = (positions[None, :] < length_row[:, None])[:, None, None, :]
        context_scores = jnp.where(seen, context_scores, mask_value)
        fresh_scores = jnp.einsum('jshl,jul->jshu', query_f, fresh_f) * score_scale
        step_ids = jnp.arange(STEPS, dtype=jnp.int32)
        fresh_seen = (step_ids[None, :] <= step_ids[:, None])[None, :, None, :]
        fresh_scores = jnp.where(fresh_seen, fresh_scores, mask_value)
        highest = jnp.maximum(lax.optimization_barrier(jnp.max(context_scores, axis=3)), lax.optimization_barrier(jnp.max(fresh_scores, axis=3)))
        context_weights = jnp.where(seen, jnp.exp(context_scores - highest[..., None]), 0.0)
        fresh_weights = jnp.where(fresh_seen, jnp.exp(fresh_scores - highest[..., None]), 0.0)
        denominator = lax.optimization_barrier(jnp.sum(context_weights, axis=3)) + lax.optimization_barrier(jnp.sum(fresh_weights, axis=3))
        context_rounded = lax.optimization_barrier(context_weights.astype(jnp.bfloat16)).astype(jnp.float32)
        fresh_rounded = lax.optimization_barrier(fresh_weights.astype(jnp.bfloat16)).astype(jnp.float32)
        combined = jnp.einsum('jsht,jct->jshc', context_rounded, context[:, :CKV, :])
        combined = combined + jnp.einsum('jshu,juc->jshc', fresh_rounded, fresh_f[:, :, :CKV])
        return (combined / denominator[..., None]).astype(jnp.bfloat16)
    attention = lax.map(one_rank, (page_rank, page_index, lengths, query_all, fresh_all))
    attention = attention.reshape(ROWS, HEADS, CKV)
    head_values = jnp.einsum('rhc,hcv->rhv', attention.astype(jnp.float32), up_value.astype(jnp.float32))
    head_values = head_values.astype(jnp.bfloat16).reshape(ROWS, HEADS * VDIM)
    attn_out = jnp.dot(head_values, out_proj, preferred_element_type=jnp.float32)
    mixed = residual.astype(jnp.float32) + attn_out
    squares = lax.optimization_barrier(jnp.mean(mixed * mixed, axis=1, keepdims=True))
    normed = (mixed * lax.rsqrt(squares + epsilon) * norm_gain).astype(jnp.bfloat16)
    gate = jnp.dot(normed, w_gate, preferred_element_type=jnp.float32)
    up_part = jnp.dot(normed, w_up, preferred_element_type=jnp.float32)
    hidden = (jax.nn.silu(gate) * up_part).astype(jnp.bfloat16)
    return (mixed + jnp.dot(hidden, w_down, preferred_element_type=jnp.float32)).astype(jnp.bfloat16)
```

```python
import functools
import math

import jax
import jax.numpy as jnp
from jax import lax
from jax.experimental import pallas as pl
from jax.experimental.pallas import tpu as pltpu
from jax.sharding import PartitionSpec as P

D = 7168
CKV = 512
PAGE = 128
CORES = 2

score_scale = 1.0 / math.sqrt(192.0)
epsilon = 1e-06
mask_value = -1e30
tiny = 1e-30

MESH = pl.DeviceIdType.MESH
f32, bf16, i32 = jnp.float32, jnp.bfloat16, jnp.int32


def split_three(value):
    first = value.astype(bf16)
    rest = value - first.astype(f32)
    second = rest.astype(bf16)
    third = (rest - second.astype(f32)).astype(bf16)
    return first, second, third


def layer_kernel(
    dp,
    rep,
    page_rank,
    page_index,
    lengths,
    queries_hbm,
    fresh_hbm,
    residual_hbm,
    gain_hbm,
    store_hbm,
    up_value_hbm,
    out_proj_hbm,
    w_gate_hbm,
    w_up_hbm,
    w_down_hbm,
    out_ref,
    query_raw,
    fresh_raw,
    residual,
    gain,
    pages,
    up_value,
    out_proj,
    w_gate,
    w_up,
    w_down,
    queries,
    own_pages,
    peer_pages,
    own_limits,
    peer_limits,
    part,
    part_recv,
    latent,
    value_buf,
    level_buf,
    op_buf,
    mixed,
    sq_buf,
    gu_buf,
    down_send,
    down_recv,
    load_sem,
    q_send,
    q_recv,
    pg_send,
    pg_recv,
    lm_send,
    lm_recv,
    p_send,
    p_recv,
    v_send,
    v_recv,
    op_send,
    op_recv,
    sq_send,
    sq_recv,
    gu_send,
    gu_recv,
    dn_send,
    dn_recv,
):
    my_rank = lax.axis_index("dp")
    my_column = lax.axis_index("rep")
    my_core = lax.rem(my_column, CORES)
    my_plane = my_column // CORES
    steps, width = residual.shape
    rows = dp * steps
    latent_width = fresh_raw.shape[1]
    slots = page_rank.shape[1]
    slot_total = slots * rep
    half = up_value.shape[0]
    head_group = half * CORES
    block = half * steps
    query_count = dp * block
    cap = own_pages.shape[1]
    vdim = up_value.shape[2]

    barrier = pltpu.get_barrier_semaphore()
    columns = [lax.rem(my_column + k, rep) for k in range(1, rep)]
    low = 1 - my_rank // (dp // 2)
    near = low * my_rank + (1 - low) * (dp - 1 - my_rank)

    def mirror(d):
        return low * d + (1 - low) * (dp - 1 - d)

    def at_least(a, b):
        return (a - b + dp) // dp

    def far_peer(j):
        p = dp - 1 - j
        return mirror(p - at_least(near, p))

    def source(i):
        j = i - 1
        other = j - dp // 2
        late = at_least(j, dp // 2)
        return mirror((1 - late) * (dp // 2 + j) + late * (other + at_least(other, near)))

    ranks = [far_peer(j) for j in range(dp - 1)]
    for peer in ranks:
        pl.semaphore_signal(barrier, inc=1, device_id={"dp": peer}, device_id_type=MESH)
    for peer in columns:
        pl.semaphore_signal(barrier, inc=1, device_id={"rep": peer}, device_id_type=MESH)

    loads = []
    for i, (start, target) in enumerate(
        (
            (queries_hbm, query_raw),
            (store_hbm.at[0], pages),
            (fresh_hbm, fresh_raw),
            (residual_hbm, residual),
            (gain_hbm, gain),
            (up_value_hbm.at[pl.ds(my_core * half, half)], up_value),
            (out_proj_hbm, out_proj),
            (w_gate_hbm, w_gate),
            (w_up_hbm, w_up),
            (w_down_hbm, w_down),
        )
    ):
        copy = pltpu.make_async_copy(start, target, load_sem.at[i])
        copy.start()
        loads.append(copy)

    def to(target, start, end, send, recv):
        return pltpu.make_async_remote_copy(
            src_ref=start,
            dst_ref=end,
            send_sem=send,
            recv_sem=recv,
            device_id=target,
            device_id_type=MESH,
        )

    def spread(start, end, send, recv):
        copies = [
            to({"rep": peer}, start, end, send.at[k], recv.at[k])
            for k, peer in enumerate(columns)
        ]
        for copy in copies:
            copy.start()
        return copies

    loads[0].wait()
    pieces = []
    for p in range(dp):
        if half * latent_width % 128 == 0:
            at = pl.ds(
                pl.multiple_of((p * head_group + my_core * half) * latent_width, 128),
                half * latent_width,
            )
            chunk = query_raw[:, at].astype(f32)
        else:
            both = query_raw[
                :, p * head_group * latent_width : (p + 1) * head_group * latent_width
            ].astype(f32)
            chunk = jnp.where(
                my_core == 0, both[:, : half * latent_width], both[:, half * latent_width :]
            )
        for s in range(steps):
            for h in range(half):
                pieces.append(chunk[s : s + 1, h * latent_width : (h + 1) * latent_width])
    for r in range(0, query_count, 16):
        queries[my_rank, r : r + 16] = jnp.concatenate(pieces[r : r + 16], axis=0).astype(bf16)

    pl.semaphore_wait(barrier, dp - 1 + rep - 1)

    q_copies = []
    for j, peer in enumerate(ranks):
        copy = to(
            {"dp": peer},
            queries.at[my_rank],
            queries.at[my_rank],
            q_send.at[j],
            q_recv.at[my_rank],
        )
        copy.start()
        q_copies.append(copy)

    partner = my_plane * CORES + (1 - my_core)
    limit_rows = lax.broadcasted_iota(i32, own_limits.shape[1:], 0)
    loads[1].wait()

    def compact(i, carry):
        d = my_rank if isinstance(i, int) and i == 0 else source(i)
        count = jnp.int32(0)
        index = [jnp.int32(0)] * cap
        limit = [jnp.int32(0)] * cap
        for q in range(slots):
            held = jnp.where(page_rank[d, q] == my_rank, 1, 0)
            place = lax.rem(my_column * slots + q, slot_total) * PAGE
            seen = jnp.clip(lengths[d, 0] - place, 0, PAGE)
            for j in range(cap):
                hit = jnp.where(count == j, held, 0)
                index[j] = index[j] + hit * page_index[d, q]
                limit[j] = limit[j] + hit * seen
            count = count + held
        levels = jnp.zeros(limit_rows.shape, i32)
        for j in range(cap):
            own_pages[d, j] = pages[index[j]]
            levels = jnp.where(limit_rows == j, limit[j], levels)
        own_limits[d] = levels
        to({"rep": partner}, own_pages.at[d], peer_pages.at[d], pg_send.at[d], pg_recv.at[d]).start()
        to(
            {"rep": partner}, own_limits.at[d], peer_limits.at[d], lm_send.at[d], lm_recv.at[d]
        ).start()
        return carry

    compact(0, 0)
    if dp <= 4:
        for i in range(1, dp):
            compact(i, 0)
    else:
        lax.fori_loop(1, dp, compact, 0)

    lanes = lax.broadcasted_iota(i32, (query_count, PAGE), 1)
    row_ids = lax.broadcasted_iota(i32, (query_count, PAGE), 0)

    def attend(i, carry):
        first = isinstance(i, int) and i == 0
        if first:
            d = my_rank
        else:
            d = source(i)
            to({"dp": d}, queries.at[d], queries.at[d], q_send.at[0], q_recv.at[d]).wait_recv()
        to(
            {"rep": partner}, own_pages.at[d], peer_pages.at[d], pg_send.at[d], pg_recv.at[d]
        ).wait_recv()
        to(
            {"rep": partner}, own_limits.at[d], peer_limits.at[d], lm_send.at[d], lm_recv.at[d]
        ).wait_recv()
        query = queries[d]
        keys, visible = [], []
        for pages_ref, limits_ref in ((own_pages, own_limits), (peer_pages, peer_limits)):
            for j in range(cap):
                keys.append(pages_ref[d, j])
                visible.append(lanes < limits_ref[d, j : j + 1, :])
        keys = jnp.concatenate(keys, axis=1)
        score = jnp.dot(query, keys, preferred_element_type=f32) * score_scale
        scores = [
            jnp.where(see, score[:, n * PAGE : (n + 1) * PAGE], mask_value)
            for n, see in enumerate(visible)
        ]
        if first:
            loads[2].wait()
            fresh = jnp.concatenate(
                [fresh_raw[...].astype(f32), jnp.zeros((PAGE - steps, latent_width), f32)], axis=0
            ).astype(bf16)
            extra = lax.dot_general(
                query, fresh, (((1,), (1,)), ((), ())), preferred_element_type=f32
            )
            step = lax.rem(row_ids, block) // half
            see = lanes + PAGE * my_plane <= step
            visible.append(see)
            scores.append(jnp.where(see, extra * score_scale, mask_value))
        peak = jnp.max(functools.reduce(jnp.maximum, scores), axis=1, keepdims=True)
        weights = [
            jnp.where(see, jnp.exp(score - peak), 0.0)
            for see, score in zip(visible, scores, strict=True)
        ]
        total = jnp.sum(functools.reduce(jnp.add, weights), axis=1, keepdims=True)
        rounded = [weight.astype(bf16) for weight in weights]
        value = lax.dot_general(
            jnp.concatenate(rounded[: CORES * cap], axis=1),
            keys[:CKV],
            (((1,), (1,)), ((), ())),
            preferred_element_type=f32,
        )
        if first:
            value += jnp.dot(rounded[-1], fresh[:, :CKV], preferred_element_type=f32)
        value = value / jnp.maximum(total, tiny)
        level = jnp.where(total > 0.0, peak + jnp.log(jnp.maximum(total, tiny)), mask_value)
        one, two, three = (term.astype(f32) for term in split_three(level))
        stat = jnp.where(lanes == 0, one, jnp.where(lanes == 1, two, three))
        for p in range(dp):
            part[i, p, :, :CKV] = value[p * block : (p + 1) * block].astype(bf16)
            part[i, p, :, CKV:] = stat[p * block : (p + 1) * block].astype(bf16)
        for peer in ranks:
            to(
                {"dp": peer},
                part.at[i, peer],
                part_recv.at[d, my_rank],
                p_send.at[i],
                p_recv.at[d],
            ).start()
        part_recv[d, my_rank] = part[i, my_rank]
        return carry

    attend(0, 0)
    if dp <= 4:
        for i in range(1, dp):
            attend(i, 0)
    else:
        lax.fori_loop(1, dp, attend, 0)

    levels = []
    for d in range(dp):
        to(
            {"dp": ranks[0]},
            part.at[0, pl.ds(0, dp - 1)],
            part_recv.at[d, pl.ds(0, dp - 1)],
            p_send.at[0],
            p_recv.at[d],
        ).wait_recv()
        message = part_recv[d].astype(f32)
        level = (
            message[:, :, CKV : CKV + 1]
            + message[:, :, CKV + 1 : CKV + 2]
            + message[:, :, CKV + 2 : CKV + 3]
        )
        best = jnp.max(level, axis=0)
        factor = jnp.exp(level - best[None])
        total = jnp.sum(factor, axis=0)
        latent[d * block : (d + 1) * block] = (
            jnp.sum(message[:, :, :CKV] * factor, axis=0) / total
        )
        levels.append(best + jnp.log(total))
    loads[5].wait()
    projected = jnp.dot(
        latent[...].astype(bf16),
        jnp.concatenate([up_value[h] for h in range(half)], axis=1),
        preferred_element_type=f32,
    )
    row_head = lax.rem(lax.broadcasted_iota(i32, (query_count, 128), 0), half)
    level = jnp.where(
        row_head == lax.broadcasted_iota(i32, (query_count, 128), 1),
        jnp.concatenate(levels, axis=0),
        0.0,
    )
    picked = jnp.concatenate(
        [
            jnp.where(row_head[:, :vdim] == h, projected[:, h * vdim : (h + 1) * vdim], 0.0)
            for h in range(half)
        ],
        axis=1,
    )
    if half > 1:
        picked = jnp.sum(picked.reshape(rows, half, half * vdim), axis=1)
        level = jnp.sum(level.reshape(rows, half, 128), axis=1)
    value_buf[my_column] = picked.astype(bf16)
    level_buf[my_column] = level
    v_copies = spread(value_buf.at[my_column], value_buf.at[my_column], v_send.at[0], v_recv.at[0])
    v_copies += spread(level_buf.at[my_column], level_buf.at[my_column], v_send.at[1], v_recv.at[1])
    for copy in v_copies:
        copy.wait()
    values = []
    for k in range(CORES):
        held = range(k, rep, CORES)
        best = functools.reduce(jnp.maximum, [level_buf[c] for c in held])
        factors = [jnp.exp(level_buf[c] - best) for c in held]
        total = functools.reduce(jnp.add, factors)
        factors = [factor / total for factor in factors]
        for h in range(half):
            values.append(
                functools.reduce(
                    jnp.add,
                    [
                        value_buf[c, :, h * vdim : (h + 1) * vdim].astype(f32)
                        * factor[:, h : h + 1]
                        for c, factor in zip(held, factors, strict=True)
                    ],
                )
            )
    values = jnp.concatenate(values, axis=1).astype(bf16)

    loads[3].wait()
    loads[6].wait()
    own_row = lax.broadcasted_iota(i32, (rows, width), 0) // steps == my_rank
    whole = jnp.where(
        own_row, jnp.concatenate([residual[...].astype(f32)] * dp, axis=0), 0.0
    ) + jnp.dot(values, out_proj[...], preferred_element_type=f32)
    op_buf[my_rank] = whole.astype(bf16)
    op_copies = []
    for j, peer in enumerate(ranks):
        item = op_buf.at[my_rank]
        copy = to({"dp": peer}, item, item, op_send.at[j], op_recv.at[my_rank])
        copy.start()
        op_copies.append(copy)
    for peer in ranks:
        item = op_buf.at[peer]
        to({"dp": peer}, item, item, op_send.at[0], op_recv.at[peer]).wait_recv()
        whole += op_buf[peer].astype(f32)
    for d in range(dp):
        mixed[d] = whole[d * steps : (d + 1) * steps]
    sq_buf[my_column] = jnp.broadcast_to(
        jnp.sum(whole * whole, axis=1, keepdims=True), (rows, 128)
    )
    sq_copies = spread(sq_buf.at[my_column], sq_buf.at[my_column], sq_send, sq_recv)
    loads[4].wait()
    scaled = (whole * gain[...].reshape(1, width)).astype(bf16)

    chunks, chunk = gu_buf.shape[1], gu_buf.shape[4]
    loads[7].wait()
    loads[8].wait()
    gu_copies = []
    for c in range(chunks):
        at = slice(c * chunk, (c + 1) * chunk)
        gu_buf[my_column, c, 0] = jnp.dot(
            scaled, w_gate[:, at], preferred_element_type=f32
        ).astype(bf16)
        gu_buf[my_column, c, 1] = jnp.dot(
            scaled, w_up[:, at], preferred_element_type=f32
        ).astype(bf16)
        item = gu_buf.at[my_column, c]
        gu_copies.append(spread(item, item, gu_send.at[c], gu_recv.at[c]))

    for copy in sq_copies:
        copy.wait()
    total = sq_buf[0]
    for c in range(1, rep):
        total += sq_buf[c]
    scale = lax.rsqrt(total[:, :1] / D + epsilon)
    loads[9].wait()
    down = jnp.zeros((rows, width), f32)
    for c in range(chunks):
        for copy in gu_copies[c]:
            copy.wait()
        gate = gu_buf[0, c, 0].astype(f32)
        up = gu_buf[0, c, 1].astype(f32)
        for other in range(1, rep):
            gate += gu_buf[other, c, 0].astype(f32)
            up += gu_buf[other, c, 1].astype(f32)
        gate = gate * scale
        up = up * scale
        hidden = (gate / (1.0 + jnp.exp(-gate)) * up).astype(bf16)
        down += jnp.dot(
            hidden, w_down[c * chunk : (c + 1) * chunk], preferred_element_type=f32
        )
    for d in range(dp):
        down_send[d] = down[d * steps : (d + 1) * steps].astype(bf16)
    dn_copies = [
        to(
            {"dp": peer},
            down_send.at[peer],
            down_recv.at[my_rank],
            dn_send.at[k],
            dn_recv.at[my_rank],
        )
        for k, peer in enumerate(ranks)
    ]
    for copy in dn_copies:
        copy.start()
    result = mixed[my_rank] + down_send[my_rank].astype(f32)

    for copy in q_copies + op_copies:
        copy.wait_send()
    for d in range(dp):
        to({"rep": partner}, own_pages.at[d], peer_pages.at[d], pg_send.at[d], pg_recv.at[d]).wait_send()
        to(
            {"rep": partner}, own_limits.at[d], peer_limits.at[d], lm_send.at[d], lm_recv.at[d]
        ).wait_send()
        to(
            {"dp": ranks[0]},
            part.at[d, pl.ds(0, dp - 1)],
            part_recv.at[0, pl.ds(0, dp - 1)],
            p_send.at[d],
            p_recv.at[0],
        ).wait_send()

    for peer in ranks:
        to(
            {"dp": peer}, down_send.at[peer], down_recv.at[peer], dn_send.at[0], dn_recv.at[peer]
        ).wait_recv()
        result += down_recv[peer].astype(f32)
    for copy in dn_copies:
        copy.wait_send()
    out_ref[...] = result.astype(bf16)


def layer(
    latent_store,
    page_rank,
    page_index,
    lengths,
    queries,
    new_latent,
    up_value,
    out_proj,
    residual,
    norm_gain,
    w_gate,
    w_up,
    w_down,
):
    dp, rep = lax.axis_size("dp"), lax.axis_size("rep")
    steps, width = residual.shape
    rows = dp * steps
    hidden_width = w_gate.shape[1]
    latent_width = new_latent.shape[1]
    slots = latent_store.shape[1]
    cap = -(-slots // dp)
    half = up_value.shape[0] // CORES
    block = half * steps
    query_count = dp * block
    vdim = up_value.shape[2]
    chunks = 3 if hidden_width % (3 * 128) == 0 else 1
    dma = pltpu.SemaphoreType.DMA
    smem = pl.BlockSpec(memory_space=pltpu.SMEM)
    hbm = pl.BlockSpec(memory_space=pl.ANY)
    return pl.pallas_call(
        functools.partial(layer_kernel, dp, rep),
        out_shape=jax.ShapeDtypeStruct((steps, width), bf16),
        in_specs=[smem] * 3 + [hbm] * 10,
        out_specs=pl.BlockSpec(memory_space=pltpu.VMEM),
        scratch_shapes=[
            pltpu.VMEM(queries.shape, bf16),
            pltpu.VMEM(new_latent.shape, bf16),
            pltpu.VMEM(residual.shape, bf16),
            pltpu.VMEM(norm_gain.shape, f32),
            pltpu.VMEM(latent_store.shape[1:], bf16),
            pltpu.VMEM((half,) + up_value.shape[1:], bf16),
            pltpu.VMEM(out_proj.shape, bf16),
            pltpu.VMEM(w_gate.shape, bf16),
            pltpu.VMEM(w_up.shape, bf16),
            pltpu.VMEM(w_down.shape, bf16),
            pltpu.VMEM((dp, query_count, latent_width), bf16),
            pltpu.VMEM((dp, cap) + latent_store.shape[2:], bf16),
            pltpu.VMEM((dp, cap) + latent_store.shape[2:], bf16),
            pltpu.VMEM((dp, 8, PAGE), i32),
            pltpu.VMEM((dp, 8, PAGE), i32),
            pltpu.VMEM((dp, dp, block, CKV + PAGE), bf16),
            pltpu.VMEM((dp, dp, block, CKV + PAGE), bf16),
            pltpu.VMEM((query_count, CKV), f32),
            pltpu.VMEM((rep, rows, half * vdim), bf16),
            pltpu.VMEM((rep, rows, 128), f32),
            pltpu.VMEM((dp, rows, width), bf16),
            pltpu.VMEM((dp, steps, width), f32),
            pltpu.VMEM((rep, rows, 128), f32),
            pltpu.VMEM((rep, chunks, 2, rows, hidden_width // chunks), bf16),
            pltpu.VMEM((dp, steps, width), bf16),
            pltpu.VMEM((dp, steps, width), bf16),
            dma((10,)),
            dma((dp - 1,)),
            dma((dp,)),
            dma((dp,)),
            dma((dp,)),
            dma((dp,)),
            dma((dp,)),
            dma((dp,)),
            dma((dp,)),
            dma((2, rep - 1)),
            dma((2, rep - 1)),
            dma((dp - 1,)),
            dma((dp,)),
            dma((rep - 1,)),
            dma((rep - 1,)),
            dma((chunks, rep - 1)),
            dma((chunks, rep - 1)),
            dma((dp - 1,)),
            dma((dp,)),
        ],
        compiler_params=pltpu.CompilerParams(
            collective_id=0, has_side_effects=True, vmem_limit_bytes=60 * 1024 * 1024
        ),
    )(
        page_rank,
        page_index,
        lengths,
        queries,
        new_latent,
        residual,
        norm_gain,
        latent_store,
        up_value,
        out_proj,
        w_gate,
        w_up,
        w_down,
    )


def solution(mesh):
    in_specs = (
        P(("groups", "dp"), "rep", None, None),
        P("groups", "rep"),
        P("groups", "rep"),
        P("groups", None),
        P(("groups", "dp"), None),
        P(("groups", "dp"), None),
        P("dp", None, None),
        P("dp", "rep"),
        P(("groups", "dp"), "rep"),
        P("rep"),
        P("rep", "dp"),
        P("rep", "dp"),
        P("dp", "rep"),
    )
    out_specs = P(("groups", "dp"), "rep")
    return jax.shard_map(
        layer, mesh=mesh, in_specs=in_specs, out_specs=out_specs, check_vma=False
    )
```

```python
import functools
import math

import jax
import jax.numpy as jnp
from jax import lax
from jax.experimental import pallas as pl
from jax.experimental.pallas import tpu as pltpu
from jax.sharding import PartitionSpec as P

D = 7168
CKV = 512
PAGE = 128
CORES = 2

score_scale = 1.0 / math.sqrt(192.0)
epsilon = 1e-06
mask_value = -1e30
tiny = 1e-30

MESH = pl.DeviceIdType.MESH
f32, bf16, i32 = jnp.float32, jnp.bfloat16, jnp.int32


def split_three(value):
    first = value.astype(bf16)
    rest = value - first.astype(f32)
    second = rest.astype(bf16)
    third = (rest - second.astype(f32)).astype(bf16)
    return first, second, third


def layer_kernel(
    dp,
    rep,
    page_rank,
    page_index,
    lengths,
    queries_hbm,
    fresh_hbm,
    residual_hbm,
    gain_hbm,
    store_hbm,
    up_value_hbm,
    out_proj_hbm,
    w_gate_hbm,
    w_up_hbm,
    w_down_hbm,
    out_ref,
    query_raw,
    fresh_raw,
    residual,
    gain,
    pages,
    up_value,
    out_proj,
    w_gate,
    w_up,
    w_down,
    queries,
    tails,
    own_pages,
    peer_pages,
    own_limits,
    peer_limits,
    part,
    part_recv,
    latent,
    value_buf,
    level_buf,
    op_buf,
    mixed,
    sq_buf,
    gu_buf,
    down_send,
    down_recv,
    load_sem,
    q_send,
    q_recv,
    t_send,
    t_recv,
    pg_send,
    pg_recv,
    lm_send,
    lm_recv,
    p_send,
    p_recv,
    v_send,
    v_recv,
    op_send,
    op_recv,
    sq_send,
    sq_recv,
    gu_send,
    gu_recv,
    dn_send,
    dn_recv,
):
    my_rank = lax.axis_index("dp")
    my_column = lax.axis_index("rep")
    my_core = lax.rem(my_column, CORES)
    my_plane = my_column // CORES
    steps, width = residual.shape
    rows = dp * steps
    latent_width = fresh_raw.shape[1]
    slots = page_rank.shape[1]
    slot_total = slots * rep
    half = up_value.shape[0]
    head_group = half * CORES
    block = half * steps
    query_count = dp * block
    cap = own_pages.shape[1]
    vdim = up_value.shape[2]

    barrier = pltpu.get_barrier_semaphore()
    columns = [lax.rem(my_column + k, rep) for k in range(1, rep)]
    bits = dp.bit_length() - 1

    def flipped(mask):
        return sum((my_rank // 2**b + mask // 2**b) % 2 * 2**b for b in range(bits))

    def source(i):
        return flipped((0, 1, 3, 2)[i] if dp == 4 else i)

    ranks = [source(i) for i in range(1, dp)]
    for peer in ranks:
        pl.semaphore_signal(barrier, inc=1, device_id={"dp": peer}, device_id_type=MESH)
    for peer in columns:
        pl.semaphore_signal(barrier, inc=1, device_id={"rep": peer}, device_id_type=MESH)

    loads = []
    for i, (start, target) in enumerate(
        (
            (queries_hbm, query_raw),
            (store_hbm.at[0], pages),
            (fresh_hbm, fresh_raw),
            (residual_hbm, residual),
            (gain_hbm, gain),
            (up_value_hbm.at[pl.ds(my_core * half, half)], up_value),
            (out_proj_hbm, out_proj),
            (w_gate_hbm, w_gate),
            (w_up_hbm, w_up),
            (w_down_hbm, w_down),
        )
    ):
        copy = pltpu.make_async_copy(start, target, load_sem.at[i])
        copy.start()
        loads.append(copy)

    def to(target, start, end, send, recv):
        return pltpu.make_async_remote_copy(
            src_ref=start,
            dst_ref=end,
            send_sem=send,
            recv_sem=recv,
            device_id=target,
            device_id_type=MESH,
        )

    def spread(start, end, send, recv):
        copies = [
            to({"rep": peer}, start, end, send.at[k], recv.at[k])
            for k, peer in enumerate(columns)
        ]
        for copy in copies:
            copy.start()
        return copies

    loads[0].wait()
    pieces = []
    for p in range(dp):
        if half * latent_width % 128 == 0:
            at = pl.ds(
                pl.multiple_of((p * head_group + my_core * half) * latent_width, 128),
                half * latent_width,
            )
            chunk = query_raw[:, at].astype(f32)
        else:
            both = query_raw[
                :, p * head_group * latent_width : (p + 1) * head_group * latent_width
            ].astype(f32)
            chunk = jnp.where(
                my_core == 0, both[:, : half * latent_width], both[:, half * latent_width :]
            )
        for s in range(steps):
            for h in range(half):
                pieces.append(chunk[s : s + 1, h * latent_width : (h + 1) * latent_width])
    tail_rows = []
    for r in range(0, query_count, 16):
        whole = jnp.concatenate(pieces[r : r + 16], axis=0)
        queries[my_rank, r : r + 16] = whole[:, :CKV].astype(bf16)
        tail_rows.append(whole[:, CKV:])
    tail = jnp.concatenate(tail_rows, axis=0)
    tails[my_rank] = jnp.concatenate(
        [tail[: query_count // 2], tail[query_count // 2 :]], axis=1
    ).astype(bf16)

    pl.semaphore_wait(barrier, dp - 1 + rep - 1)

    def query_copies(peer, d, j):
        return (
            to({"dp": peer}, queries.at[d], queries.at[d], q_send.at[j], q_recv.at[d]),
            to({"dp": peer}, tails.at[d], tails.at[d], t_send.at[j], t_recv.at[d]),
        )

    q_copies = []
    for j, peer in enumerate(ranks):
        for copy in query_copies(peer, my_rank, j):
            copy.start()
            q_copies.append(copy)

    partner = my_plane * CORES + (1 - my_core)
    limit_rows = lax.broadcasted_iota(i32, own_limits.shape[1:], 0)
    loads[1].wait()

    def page_copies(d):
        return (
            to({"rep": partner}, own_pages.at[d], peer_pages.at[d], pg_send.at[d], pg_recv.at[d]),
            to(
                {"rep": partner}, own_limits.at[d], peer_limits.at[d], lm_send.at[d], lm_recv.at[d]
            ),
        )

    def compact(i, carry):
        d = source(i)
        count = jnp.int32(0)
        index = [jnp.int32(0)] * cap
        limit = [jnp.int32(0)] * cap
        for q in range(slots):
            held = jnp.where(page_rank[d, q] == my_rank, 1, 0)
            place = lax.rem(my_column * slots + q, slot_total) * PAGE
            seen = jnp.clip(lengths[0, d] - place, 0, PAGE)
            for j in range(cap):
                hit = jnp.where(count == j, held, 0)
                index[j] = index[j] + hit * page_index[d, q]
                limit[j] = limit[j] + hit * seen
            count = count + held
        levels = jnp.zeros(limit_rows.shape, i32)
        for j in range(cap):
            own_pages[d, j] = pages[index[j]]
            levels = jnp.where(limit_rows == j, limit[j], levels)
        own_limits[d] = levels
        for copy in page_copies(d):
            copy.start()
        return carry

    compact(0, 0)
    if dp <= 4:
        for i in range(1, dp):
            compact(i, 0)
    else:
        lax.fori_loop(1, dp, compact, 0)

    lanes = lax.broadcasted_iota(i32, (query_count, PAGE), 1)
    row_ids = lax.broadcasted_iota(i32, (query_count, PAGE), 0)

    def send_part(i):
        d = source(i)
        for peer in ranks:
            to(
                {"dp": peer},
                part.at[i, peer],
                part_recv.at[d, my_rank],
                p_send.at[i],
                p_recv.at[d],
            ).start()

    def attend(i, carry):
        first = isinstance(i, int) and i == 0
        d = source(i)
        if not first:
            for copy in query_copies(d, d, 0):
                copy.wait_recv()
        for copy in page_copies(d):
            copy.wait_recv()
        if not first and isinstance(i, int) and i == 1:
            send_part(0)
        query = queries[d]
        tail = tails[d].astype(f32)
        tail = jnp.concatenate(
            [tail[:, : latent_width - CKV], tail[:, latent_width - CKV :]], axis=0
        ).astype(bf16)
        keys, visible = [], []
        for pages_ref, limits_ref in ((own_pages, own_limits), (peer_pages, peer_limits)):
            for j in range(cap):
                keys.append(pages_ref[d, j])
                visible.append(lanes < limits_ref[d, j : j + 1, :])
        keys = jnp.concatenate(keys, axis=1)
        score = (
            jnp.dot(query, keys[:CKV], preferred_element_type=f32)
            + jnp.dot(tail, keys[CKV:], preferred_element_type=f32)
        ) * score_scale
        scores = [
            jnp.where(see, score[:, n * PAGE : (n + 1) * PAGE], mask_value)
            for n, see in enumerate(visible)
        ]
        if first:
            loads[2].wait()
            fresh = jnp.concatenate(
                [fresh_raw[...].astype(f32), jnp.zeros((PAGE - steps, latent_width), f32)], axis=0
            ).astype(bf16)
            across = (((1,), (1,)), ((), ()))
            extra = lax.dot_general(
                query, fresh[:, :CKV], across, preferred_element_type=f32
            ) + lax.dot_general(tail, fresh[:, CKV:], across, preferred_element_type=f32)
            step = lax.rem(row_ids, block) // half
            see = lanes + PAGE * my_plane <= step
            visible.append(see)
            scores.append(jnp.where(see, extra * score_scale, mask_value))
        peak = jnp.max(functools.reduce(jnp.maximum, scores), axis=1, keepdims=True)
        weights = [
            jnp.where(see, jnp.exp(score - peak), 0.0)
            for see, score in zip(visible, scores, strict=True)
        ]
        total = jnp.sum(functools.reduce(jnp.add, weights), axis=1, keepdims=True)
        rounded = [weight.astype(bf16) for weight in weights]
        value = lax.dot_general(
            jnp.concatenate(rounded[: CORES * cap], axis=1),
            keys[:CKV],
            (((1,), (1,)), ((), ())),
            preferred_element_type=f32,
        )
        if first:
            value += jnp.dot(rounded[-1], fresh[:, :CKV], preferred_element_type=f32)
        value = value / jnp.maximum(total, tiny)
        level = jnp.where(total > 0.0, peak + jnp.log(jnp.maximum(total, tiny)), mask_value)
        one, two, three = (term.astype(f32) for term in split_three(level))
        stat = jnp.where(lanes == 0, one, jnp.where(lanes == 1, two, three))
        for p in range(dp):
            part[i, p, :, :CKV] = value[p * block : (p + 1) * block].astype(bf16)
            part[i, p, :, CKV:] = stat[p * block : (p + 1) * block].astype(bf16)
        if not first:
            send_part(i)
        part_recv[d, my_rank] = part[i, my_rank]
        return carry

    attend(0, 0)
    if dp <= 4:
        for i in range(1, dp):
            attend(i, 0)
    else:
        send_part(0)
        lax.fori_loop(1, dp, attend, 0)

    levels = []
    for d in range(dp):
        to(
            {"dp": ranks[0]},
            part.at[0, pl.ds(0, dp - 1)],
            part_recv.at[d, pl.ds(0, dp - 1)],
            p_send.at[0],
            p_recv.at[d],
        ).wait_recv()
    for d in range(dp):
        message = part_recv[d].astype(f32)
        level = (
            message[:, :, CKV : CKV + 1]
            + message[:, :, CKV + 1 : CKV + 2]
            + message[:, :, CKV + 2 : CKV + 3]
        )
        best = jnp.max(level, axis=0)
        factor = jnp.exp(level - best[None])
        total = jnp.sum(factor, axis=0)
        latent[d * block : (d + 1) * block] = (
            jnp.sum(message[:, :, :CKV] * factor, axis=0) / total
        )
        levels.append(best + jnp.log(total))
    loads[5].wait()
    projected = jnp.dot(
        latent[...].astype(bf16),
        jnp.concatenate([up_value[h] for h in range(half)], axis=1),
        preferred_element_type=f32,
    )
    row_head = lax.rem(lax.broadcasted_iota(i32, (query_count, 128), 0), half)
    level = jnp.where(
        row_head == lax.broadcasted_iota(i32, (query_count, 128), 1),
        jnp.concatenate(levels, axis=0),
        0.0,
    )
    picked = jnp.concatenate(
        [
            jnp.where(row_head[:, :vdim] == h, projected[:, h * vdim : (h + 1) * vdim], 0.0)
            for h in range(half)
        ],
        axis=1,
    )
    if half > 1:
        picked = jnp.sum(picked.reshape(rows, half, half * vdim), axis=1)
        level = jnp.sum(level.reshape(rows, half, 128), axis=1)
    value_buf[my_column] = picked.astype(bf16)
    level_buf[my_column] = level
    v_copies = spread(value_buf.at[my_column], value_buf.at[my_column], v_send.at[0], v_recv.at[0])
    v_copies += spread(level_buf.at[my_column], level_buf.at[my_column], v_send.at[1], v_recv.at[1])
    for copy in v_copies:
        copy.wait()
    values = []
    for k in range(CORES):
        held = range(k, rep, CORES)
        best = functools.reduce(jnp.maximum, [level_buf[c] for c in held])
        factors = [jnp.exp(level_buf[c] - best) for c in held]
        total = functools.reduce(jnp.add, factors)
        factors = [factor / total for factor in factors]
        for h in range(half):
            values.append(
                functools.reduce(
                    jnp.add,
                    [
                        value_buf[c, :, h * vdim : (h + 1) * vdim].astype(f32)
                        * factor[:, h : h + 1]
                        for c, factor in zip(held, factors, strict=True)
                    ],
                )
            )
    values = jnp.concatenate(values, axis=1).astype(bf16)

    loads[3].wait()
    loads[6].wait()
    own_row = lax.broadcasted_iota(i32, (rows, width), 0) // steps == my_rank
    whole = jnp.where(
        own_row, jnp.concatenate([residual[...].astype(f32)] * dp, axis=0), 0.0
    ) + jnp.dot(values, out_proj[...], preferred_element_type=f32)
    op_buf[my_rank] = whole.astype(bf16)
    op_copies = []
    for j, peer in enumerate(ranks):
        item = op_buf.at[my_rank]
        copy = to({"dp": peer}, item, item, op_send.at[j], op_recv.at[my_rank])
        copy.start()
        op_copies.append(copy)
    for peer in ranks:
        item = op_buf.at[peer]
        to({"dp": peer}, item, item, op_send.at[0], op_recv.at[peer]).wait_recv()
        whole += op_buf[peer].astype(f32)
    for d in range(dp):
        mixed[d] = whole[d * steps : (d + 1) * steps]
    sq_buf[my_column] = jnp.broadcast_to(
        jnp.sum(whole * whole, axis=1, keepdims=True), (rows, 128)
    )
    sq_copies = spread(sq_buf.at[my_column], sq_buf.at[my_column], sq_send, sq_recv)
    loads[4].wait()
    scaled = (whole * gain[...].reshape(1, width)).astype(bf16)

    chunks, chunk = gu_buf.shape[1], gu_buf.shape[4]
    loads[7].wait()
    loads[8].wait()
    gu_copies = []
    for c in range(chunks):
        at = slice(c * chunk, (c + 1) * chunk)
        gu_buf[my_column, c, 0] = jnp.dot(
            scaled, w_gate[:, at], preferred_element_type=f32
        ).astype(bf16)
        gu_buf[my_column, c, 1] = jnp.dot(
            scaled, w_up[:, at], preferred_element_type=f32
        ).astype(bf16)
        item = gu_buf.at[my_column, c]
        gu_copies.append(spread(item, item, gu_send.at[c], gu_recv.at[c]))

    for copy in sq_copies:
        copy.wait()
    total = sq_buf[0]
    for c in range(1, rep):
        total += sq_buf[c]
    scale = lax.rsqrt(total[:, :1] / D + epsilon)
    loads[9].wait()
    down = jnp.zeros((rows, width), f32)
    for c in range(chunks):
        for copy in gu_copies[c]:
            copy.wait()
        gate = gu_buf[0, c, 0].astype(f32)
        up = gu_buf[0, c, 1].astype(f32)
        for other in range(1, rep):
            gate += gu_buf[other, c, 0].astype(f32)
            up += gu_buf[other, c, 1].astype(f32)
        gate = gate * scale
        up = up * scale
        hidden = (gate / (1.0 + jnp.exp(-gate)) * up).astype(bf16)
        down += jnp.dot(
            hidden, w_down[c * chunk : (c + 1) * chunk], preferred_element_type=f32
        )
    for d in range(dp):
        down_send[d] = down[d * steps : (d + 1) * steps].astype(bf16)
    dn_copies = [
        to(
            {"dp": peer},
            down_send.at[peer],
            down_recv.at[my_rank],
            dn_send.at[k],
            dn_recv.at[my_rank],
        )
        for k, peer in enumerate(ranks)
    ]
    for copy in dn_copies:
        copy.start()
    result = mixed[my_rank] + down_send[my_rank].astype(f32)

    for copy in q_copies + op_copies:
        copy.wait_send()
    for d in range(dp):
        for copy in page_copies(d):
            copy.wait_send()
        to(
            {"dp": ranks[0]},
            part.at[d, pl.ds(0, dp - 1)],
            part_recv.at[0, pl.ds(0, dp - 1)],
            p_send.at[d],
            p_recv.at[0],
        ).wait_send()

    for peer in ranks:
        to(
            {"dp": peer}, down_send.at[peer], down_recv.at[peer], dn_send.at[0], dn_recv.at[peer]
        ).wait_recv()
        result += down_recv[peer].astype(f32)
    for copy in dn_copies:
        copy.wait_send()
    out_ref[...] = result


def layer(
    latent_store,
    page_rank,
    page_index,
    lengths,
    queries,
    new_latent,
    up_value,
    out_proj,
    residual,
    norm_gain,
    w_gate,
    w_up,
    w_down,
):
    dp, rep = lax.axis_size("dp"), lax.axis_size("rep")
    steps, width = residual.shape
    rows = dp * steps
    hidden_width = w_gate.shape[1]
    latent_width = new_latent.shape[1]
    slots = latent_store.shape[1]
    cap = -(-slots // dp)
    half = up_value.shape[0] // CORES
    block = half * steps
    query_count = dp * block
    vdim = up_value.shape[2]
    chunks = hidden_width // (512 if hidden_width % 512 == 0 else 128)
    dma = pltpu.SemaphoreType.DMA
    smem = pl.BlockSpec(memory_space=pltpu.SMEM)
    hbm = pl.BlockSpec(memory_space=pl.ANY)
    return pl.pallas_call(
        functools.partial(layer_kernel, dp, rep),
        out_shape=jax.ShapeDtypeStruct((steps, width), f32),
        in_specs=[smem] * 3 + [hbm] * 10,
        out_specs=pl.BlockSpec(memory_space=pltpu.VMEM),
        scratch_shapes=[
            pltpu.VMEM(queries.shape, bf16),
            pltpu.VMEM(new_latent.shape, bf16),
            pltpu.VMEM(residual.shape, bf16),
            pltpu.VMEM(norm_gain.shape, f32),
            pltpu.VMEM(latent_store.shape[1:], bf16),
            pltpu.VMEM((half,) + up_value.shape[1:], bf16),
            pltpu.VMEM(out_proj.shape, bf16),
            pltpu.VMEM(w_gate.shape, bf16),
            pltpu.VMEM(w_up.shape, bf16),
            pltpu.VMEM(w_down.shape, bf16),
            pltpu.VMEM((dp, query_count, CKV), bf16),
            pltpu.VMEM((dp, query_count // 2, 2 * (latent_width - CKV)), bf16),
            pltpu.VMEM((dp, cap) + latent_store.shape[2:], bf16),
            pltpu.VMEM((dp, cap) + latent_store.shape[2:], bf16),
            pltpu.VMEM((dp, 8, PAGE), i32),
            pltpu.VMEM((dp, 8, PAGE), i32),
            pltpu.VMEM((dp, dp, block, CKV + PAGE), bf16),
            pltpu.VMEM((dp, dp, block, CKV + PAGE), bf16),
            pltpu.VMEM((query_count, CKV), f32),
            pltpu.VMEM((rep, rows, half * vdim), bf16),
            pltpu.VMEM((rep, rows, 128), f32),
            pltpu.VMEM((dp, rows, width), bf16),
            pltpu.VMEM((dp, steps, width), f32),
            pltpu.VMEM((rep, rows, 128), f32),
            pltpu.VMEM((rep, chunks, 2, rows, hidden_width // chunks), bf16),
            pltpu.VMEM((dp, steps, width), bf16),
            pltpu.VMEM((dp, steps, width), bf16),
            dma((10,)),
            dma((dp - 1,)),
            dma((dp,)),
            dma((dp - 1,)),
            dma((dp,)),
            dma((dp,)),
            dma((dp,)),
            dma((dp,)),
            dma((dp,)),
            dma((dp,)),
            dma((dp,)),
            dma((2, rep - 1)),
            dma((2, rep - 1)),
            dma((dp - 1,)),
            dma((dp,)),
            dma((rep - 1,)),
            dma((rep - 1,)),
            dma((chunks, rep - 1)),
            dma((chunks, rep - 1)),
            dma((dp - 1,)),
            dma((dp,)),
        ],
        compiler_params=pltpu.CompilerParams(
            collective_id=0, has_side_effects=True, vmem_limit_bytes=60 * 1024 * 1024
        ),
    )(
        page_rank,
        page_index,
        lengths.T,
        queries,
        new_latent,
        residual,
        norm_gain,
        latent_store,
        up_value,
        out_proj,
        w_gate,
        w_up,
        w_down,
    ).astype(bf16)


def solution(mesh):
    in_specs = (
        P(("groups", "dp"), "rep", None, None),
        P("groups", "rep"),
        P("groups", "rep"),
        P("groups", None),
        P(("groups", "dp"), None),
        P(("groups", "dp"), None),
        P("dp", None, None),
        P("dp", "rep"),
        P(("groups", "dp"), "rep"),
        P("rep"),
        P("rep", "dp"),
        P("rep", "dp"),
        P("dp", "rep"),
    )
    out_specs = P(("groups", "dp"), "rep")
    return jax.shard_map(
        layer, mesh=mesh, in_specs=in_specs, out_specs=out_specs, check_vma=False
    )
```

```python
import functools
import math

import jax
import jax.numpy as jnp
from jax import lax
from jax.experimental import pallas as pl
from jax.experimental.pallas import tpu as pltpu
from jax.sharding import PartitionSpec as P

D = 7168
CKV = 512
PAGE = 128
CORES = 2

score_scale = 1.0 / math.sqrt(192.0)
epsilon = 1e-06
mask_value = -1e30
tiny = 1e-30

MESH = pl.DeviceIdType.MESH
f32, bf16, i32 = jnp.float32, jnp.bfloat16, jnp.int32


def split_three(value):
    first = value.astype(bf16)
    rest = value - first.astype(f32)
    second = rest.astype(bf16)
    third = (rest - second.astype(f32)).astype(bf16)
    return first, second, third


def layer_kernel(
    dp,
    rep,
    page_rank_hbm,
    page_index_hbm,
    lengths_hbm,
    queries_hbm,
    fresh_hbm,
    residual_hbm,
    gain_hbm,
    store_hbm,
    up_value_hbm,
    out_proj_hbm,
    w_gate_hbm,
    w_up_hbm,
    w_down_hbm,
    out_ref,
    page_rank,
    page_index,
    lengths,
    query_raw,
    fresh_raw,
    residual,
    gain,
    pages,
    up_value,
    out_proj,
    w_gate,
    w_up,
    w_down,
    queries,
    tails,
    own_pages,
    peer_pages,
    own_limits,
    peer_limits,
    part,
    part_recv,
    latent,
    value_buf,
    level_buf,
    op_first,
    op_second,
    mixed,
    sq_buf,
    gu_sum,
    gu_buf,
    down_send,
    down_recv,
    load_sem,
    q_send,
    q_recv,
    t_send,
    t_recv,
    x_send,
    x_recv,
    pg_send,
    pg_recv,
    lm_send,
    lm_recv,
    p_send,
    p_recv,
    v_send,
    v_recv,
    op_send,
    op_recv,
    sq_send,
    sq_recv,
    gu_send,
    gu_recv,
    dn_send,
    dn_recv,
):
    my_rank = lax.axis_index("dp")
    my_column = lax.axis_index("rep")
    my_core = lax.rem(my_column, CORES)
    my_plane = my_column // CORES
    steps, width = residual.shape
    rows = dp * steps
    latent_width = fresh_raw.shape[1]
    slots = page_rank.shape[1]
    slot_total = slots * rep
    half = up_value.shape[0]
    head_group = half * CORES
    block = half * steps
    query_count = dp * block
    cap = own_pages.shape[1]
    vdim = up_value.shape[2]

    barrier = pltpu.get_barrier_semaphore()
    columns = [lax.rem(my_column + k, rep) for k in range(1, rep)]
    bits = dp.bit_length() - 1

    def flipped(mask):
        return sum((my_rank // 2**b + mask // 2**b) % 2 * 2**b for b in range(bits))

    def source(i):
        return flipped((0, 1, 3, 2)[i] if dp == 4 else i)

    ranks = [source(i) for i in range(1, dp)]
    for peer in ranks:
        pl.semaphore_signal(barrier, inc=1, device_id={"dp": peer}, device_id_type=MESH)
    for peer in columns:
        pl.semaphore_signal(barrier, inc=1, device_id={"rep": peer}, device_id_type=MESH)

    loads = []
    for i, (start, target) in enumerate(
        (
            (queries_hbm, query_raw),
            (store_hbm.at[0], pages),
            (fresh_hbm, fresh_raw),
            (residual_hbm, residual),
            (gain_hbm, gain),
            (up_value_hbm.at[pl.ds(my_core * half, half)], up_value),
            (out_proj_hbm, out_proj),
            (w_gate_hbm, w_gate),
            (w_up_hbm, w_up),
            (w_down_hbm, w_down),
            (page_rank_hbm, page_rank),
            (page_index_hbm, page_index),
            (lengths_hbm, lengths),
        )
    ):
        loads.append(pltpu.make_async_copy(start, target, load_sem.at[i]))
    for i in (0, 10, 11, 12, *range(1, 10)):
        loads[i].start()

    def to(target, start, end, send, recv):
        return pltpu.make_async_remote_copy(
            src_ref=start,
            dst_ref=end,
            send_sem=send,
            recv_sem=recv,
            device_id=target,
            device_id_type=MESH,
        )

    def spread(start, end, send, recv):
        copies = [
            to({"rep": peer}, start, end, send.at[k], recv.at[k])
            for k, peer in enumerate(columns)
        ]
        for copy in copies:
            copy.start()
        return copies

    loads[0].wait()
    pieces = []
    for p in range(dp):
        if half * latent_width % 128 == 0:
            at = pl.ds(
                pl.multiple_of((p * head_group + my_core * half) * latent_width, 128),
                half * latent_width,
            )
            chunk = query_raw[:, at].astype(f32)
        else:
            both = query_raw[
                :, p * head_group * latent_width : (p + 1) * head_group * latent_width
            ].astype(f32)
            chunk = jnp.where(
                my_core == 0, both[:, : half * latent_width], both[:, half * latent_width :]
            )
        for s in range(steps):
            for h in range(half):
                pieces.append(chunk[s : s + 1, h * latent_width : (h + 1) * latent_width])
    planes, share = queries.shape[1:3]
    for x in range(planes):
        whole = jnp.concatenate(pieces[x * share : (x + 1) * share], axis=0)
        queries[my_rank, x] = whole[:, :CKV].astype(bf16)
        tails[my_rank, x] = jnp.concatenate(
            [whole[: share // 2, CKV:], whole[share // 2 :, CKV:]], axis=1
        ).astype(bf16)

    pl.semaphore_wait(barrier, dp - 1 + rep - 1)

    def query_copies(peer, d, j):
        return [
            to({"dp": peer}, item.at[d, my_plane], item.at[d, my_plane], send.at[j], recv.at[d])
            for item, send, recv in ((queries, q_send, q_recv), (tails, t_send, t_recv))
        ]

    def plane_copies(d, i, arriving):
        copies = []
        for j in range(1, planes):
            peer = lax.rem(my_plane + j, planes) * CORES + my_core
            x = lax.rem(my_plane + planes - j, planes) if arriving else my_plane
            for n, item in enumerate((queries, tails)):
                copies.append(
                    to(
                        {"rep": peer},
                        item.at[d, x],
                        item.at[d, x],
                        x_send.at[n, i, j - 1],
                        x_recv.at[n, d, j - 1],
                    )
                )
        return copies

    q_copies = []
    for j, peer in enumerate(ranks):
        for copy in query_copies(peer, my_rank, j):
            copy.start()
            q_copies.append(copy)

    partner = my_plane * CORES + (1 - my_core)
    limit_rows = lax.broadcasted_iota(i32, own_limits.shape[1:], 0)
    for i in (1, 10, 11, 12):
        loads[i].wait()

    def page_copies(d):
        return (
            to({"rep": partner}, own_pages.at[d], peer_pages.at[d], pg_send.at[d], pg_recv.at[d]),
            to(
                {"rep": partner}, own_limits.at[d], peer_limits.at[d], lm_send.at[d], lm_recv.at[d]
            ),
        )

    def compact(i, carry):
        d = source(i)
        count = jnp.int32(0)
        index = [jnp.int32(0)] * cap
        limit = [jnp.int32(0)] * cap
        for q in range(slots):
            held = jnp.where(page_rank[d, q] == my_rank, 1, 0)
            place = lax.rem(my_column * slots + q, slot_total) * PAGE
            seen = jnp.clip(lengths[0, d] - place, 0, PAGE)
            for j in range(cap):
                hit = jnp.where(count == j, held, 0)
                index[j] = index[j] + hit * page_index[d, q]
                limit[j] = limit[j] + hit * seen
            count = count + held
        levels = jnp.zeros(limit_rows.shape, i32)
        for j in range(cap):
            own_pages[d, j] = pages[index[j]]
            levels = jnp.where(limit_rows == j, limit[j], levels)
        own_limits[d] = levels
        for copy in page_copies(d):
            copy.start()
        return carry

    compact(0, 0)
    if dp <= 4:
        for i in range(1, dp):
            compact(i, 0)
    else:
        lax.fori_loop(1, dp, compact, 0)

    lanes = lax.broadcasted_iota(i32, (query_count, PAGE), 1)
    row_ids = lax.broadcasted_iota(i32, (query_count, PAGE), 0)

    def send_part(i):
        d = source(i)
        for peer in ranks:
            to(
                {"dp": peer},
                part.at[i, peer],
                part_recv.at[d, my_rank],
                p_send.at[i],
                p_recv.at[d],
            ).start()

    def attend(i, carry):
        first = isinstance(i, int) and i == 0
        d = source(i)
        if not first:
            for copy in plane_copies(d, i, True):
                copy.wait_recv()
        for copy in page_copies(d):
            copy.wait_recv()
        query = queries[d].reshape(query_count, CKV)
        tail = [tails[d, x].astype(f32) for x in range(planes)]
        tail = jnp.concatenate(
            [
                item
                for pair in tail
                for item in (pair[:, : latent_width - CKV], pair[:, latent_width - CKV :])
            ],
            axis=0,
        ).astype(bf16)
        keys, visible = [], []
        for pages_ref, limits_ref in ((own_pages, own_limits), (peer_pages, peer_limits)):
            for j in range(cap):
                keys.append(pages_ref[d, j])
                visible.append(lanes < limits_ref[d, j : j + 1, :])
        keys = jnp.concatenate(keys, axis=1)
        score = (
            jnp.dot(query, keys[:CKV], preferred_element_type=f32)
            + jnp.dot(tail, keys[CKV:], preferred_element_type=f32)
        ) * score_scale
        scores = [
            jnp.where(see, score[:, n * PAGE : (n + 1) * PAGE], mask_value)
            for n, see in enumerate(visible)
        ]
        if first:
            loads[2].wait()
            fresh = jnp.concatenate(
                [fresh_raw[...].astype(f32), jnp.zeros((PAGE - steps, latent_width), f32)], axis=0
            ).astype(bf16)
            across = (((1,), (1,)), ((), ()))
            extra = lax.dot_general(
                query, fresh[:, :CKV], across, preferred_element_type=f32
            ) + lax.dot_general(tail, fresh[:, CKV:], across, preferred_element_type=f32)
            step = lax.rem(row_ids, block) // half
            see = lanes + PAGE * my_plane <= step
            visible.append(see)
            scores.append(jnp.where(see, extra * score_scale, mask_value))
        peak = jnp.max(functools.reduce(jnp.maximum, scores), axis=1, keepdims=True)
        weights = [
            jnp.where(see, jnp.exp(score - peak), 0.0)
            for see, score in zip(visible, scores, strict=True)
        ]
        total = jnp.sum(functools.reduce(jnp.add, weights), axis=1, keepdims=True)
        rounded = [weight.astype(bf16) for weight in weights]
        value = lax.dot_general(
            jnp.concatenate(rounded[: CORES * cap], axis=1),
            keys[:CKV],
            (((1,), (1,)), ((), ())),
            preferred_element_type=f32,
        )
        if first:
            value += jnp.dot(rounded[-1], fresh[:, :CKV], preferred_element_type=f32)
        value = value / jnp.maximum(total, tiny)
        level = jnp.where(total > 0.0, peak + jnp.log(jnp.maximum(total, tiny)), mask_value)
        one, two, three = (term.astype(f32) for term in split_three(level))
        stat = jnp.where(lanes == 0, one, jnp.where(lanes == 1, two, three))
        for p in range(dp):
            part[i, p, :, :CKV] = value[p * block : (p + 1) * block].astype(bf16)
            part[i, p, :, CKV:] = stat[p * block : (p + 1) * block].astype(bf16)
        send_part(i)
        part_recv[d, my_rank] = part[i, my_rank]
        return carry

    def forward(i, carry):
        d = source(i)
        for copy in query_copies(d, d, 0):
            copy.wait_recv()
        for copy in plane_copies(d, i, False):
            copy.start()
        return carry

    def for_others(step):
        if dp <= 4:
            for i in range(1, dp):
                step(i, 0)
        else:
            lax.fori_loop(1, dp, step, 0)

    attend(0, 0)
    for_others(forward)
    for_others(attend)

    levels = []
    for d in range(dp):
        to(
            {"dp": ranks[0]},
            part.at[0, pl.ds(0, dp - 1)],
            part_recv.at[d, pl.ds(0, dp - 1)],
            p_send.at[0],
            p_recv.at[d],
        ).wait_recv()
    for d in range(dp):
        message = part_recv[d].astype(f32)
        level = (
            message[:, :, CKV : CKV + 1]
            + message[:, :, CKV + 1 : CKV + 2]
            + message[:, :, CKV + 2 : CKV + 3]
        )
        best = jnp.max(level, axis=0)
        factor = jnp.exp(level - best[None])
        total = jnp.sum(factor, axis=0)
        latent[d * block : (d + 1) * block] = (
            jnp.sum(message[:, :, :CKV] * factor, axis=0) / total
        )
        levels.append(best + jnp.log(total))
    loads[5].wait()
    projected = jnp.dot(
        latent[...].astype(bf16),
        jnp.concatenate([up_value[h] for h in range(half)], axis=1),
        preferred_element_type=f32,
    )
    row_head = lax.rem(lax.broadcasted_iota(i32, (query_count, 128), 0), half)
    level = jnp.where(
        row_head == lax.broadcasted_iota(i32, (query_count, 128), 1),
        jnp.concatenate(levels, axis=0),
        0.0,
    )
    picked = jnp.concatenate(
        [
            jnp.where(row_head[:, :vdim] == h, projected[:, h * vdim : (h + 1) * vdim], 0.0)
            for h in range(half)
        ],
        axis=1,
    )
    if half > 1:
        picked = jnp.sum(picked.reshape(rows, half, half * vdim), axis=1)
        level = jnp.sum(level.reshape(rows, half, 128), axis=1)
    value_buf[my_column] = picked.astype(bf16)
    level_buf[my_column] = level
    v_copies = spread(value_buf.at[my_column], value_buf.at[my_column], v_send.at[0], v_recv.at[0])
    v_copies += spread(level_buf.at[my_column], level_buf.at[my_column], v_send.at[1], v_recv.at[1])
    for copy in v_copies:
        copy.wait()
    values = []
    for k in range(CORES):
        held = range(k, rep, CORES)
        best = functools.reduce(jnp.maximum, [level_buf[c] for c in held])
        factors = [jnp.exp(level_buf[c] - best) for c in held]
        total = functools.reduce(jnp.add, factors)
        factors = [factor / total for factor in factors]
        for h in range(half):
            values.append(
                functools.reduce(
                    jnp.add,
                    [
                        value_buf[c, :, h * vdim : (h + 1) * vdim].astype(f32)
                        * factor[:, h : h + 1]
                        for c, factor in zip(held, factors, strict=True)
                    ],
                )
            )
    values = jnp.concatenate(values, axis=1).astype(bf16)

    loads[3].wait()
    loads[6].wait()
    own_row = lax.broadcasted_iota(i32, (rows, 1), 0) // steps == my_rank
    kept = jnp.concatenate([residual[...].astype(f32)] * dp, axis=0)
    split = op_first.shape[2]
    spans = ((0, split, op_first), (split, width, op_second))
    parts, op_copies = [], []
    for n, (begin, end, buffer) in enumerate(spans):
        piece = jnp.where(own_row, kept[:, begin:end], 0.0) + jnp.dot(
            values, out_proj[:, begin:end], preferred_element_type=f32
        )
        buffer[my_rank] = piece.astype(bf16)
        parts.append(piece)
        for j, peer in enumerate(ranks):
            item = buffer.at[my_rank]
            copy = to({"dp": peer}, item, item, op_send.at[n, j], op_recv.at[n, my_rank])
            copy.start()
            op_copies.append(copy)
    loads[4].wait()
    gains = gain[...].reshape(1, width)
    chunks, chunk = gu_buf.shape[1], gu_buf.shape[4]
    loads[7].wait()
    loads[8].wait()
    squares = jnp.zeros((rows, 1), f32)
    gu_copies = []
    for n, (begin, end, buffer) in enumerate(spans):
        piece = parts[n]
        for peer in ranks:
            item = buffer.at[peer]
            to({"dp": peer}, item, item, op_send.at[n, 0], op_recv.at[n, peer]).wait_recv()
            piece += buffer[peer].astype(f32)
        for d in range(dp):
            mixed[d, :, begin:end] = piece[d * steps : (d + 1) * steps]
        squares += jnp.sum(piece * piece, axis=1, keepdims=True)
        scaled = (piece * gains[:, begin:end]).astype(bf16)
        last = n == len(spans) - 1
        if last:
            sq_buf[my_column] = jnp.broadcast_to(squares, (rows, 128))
            sq_copies = spread(sq_buf.at[my_column], sq_buf.at[my_column], sq_send, sq_recv)
        for c in range(chunks):
            at = slice(c * chunk, (c + 1) * chunk)
            for m, weight in enumerate((w_gate, w_up)):
                total = jnp.dot(scaled, weight[begin:end, at], preferred_element_type=f32)
                if n > 0:
                    total += gu_sum[m, :, at]
                if last:
                    gu_buf[my_column, c, m] = total.astype(bf16)
                else:
                    gu_sum[m, :, at] = total
            if last:
                item = gu_buf.at[my_column, c]
                gu_copies.append(spread(item, item, gu_send.at[c], gu_recv.at[c]))

    for copy in sq_copies:
        copy.wait()
    total = sq_buf[0]
    for c in range(1, rep):
        total += sq_buf[c]
    scale = lax.rsqrt(total[:, :1] / D + epsilon)
    loads[9].wait()
    down = jnp.zeros((rows, width), f32)
    for c in range(chunks):
        for copy in gu_copies[c]:
            copy.wait()
        gate = gu_buf[0, c, 0].astype(f32)
        up = gu_buf[0, c, 1].astype(f32)
        for other in range(1, rep):
            gate += gu_buf[other, c, 0].astype(f32)
            up += gu_buf[other, c, 1].astype(f32)
        gate = gate * scale
        up = up * scale
        hidden = (gate / (1.0 + jnp.exp(-gate)) * up).astype(bf16)
        down += jnp.dot(
            hidden, w_down[c * chunk : (c + 1) * chunk], preferred_element_type=f32
        )
    for d in range(dp):
        down_send[d] = down[d * steps : (d + 1) * steps].astype(bf16)
    dn_copies = [
        to(
            {"dp": peer},
            down_send.at[peer],
            down_recv.at[my_rank],
            dn_send.at[k],
            dn_recv.at[my_rank],
        )
        for k, peer in enumerate(ranks)
    ]
    for copy in dn_copies:
        copy.start()
    result = mixed[my_rank] + down_send[my_rank].astype(f32)

    for copy in q_copies + op_copies:
        copy.wait_send()
    for d in range(dp):
        for copy in page_copies(d):
            copy.wait_send()
        if d > 0:
            for copy in plane_copies(d, d, False):
                copy.wait_send()
        to(
            {"dp": ranks[0]},
            part.at[d, pl.ds(0, dp - 1)],
            part_recv.at[0, pl.ds(0, dp - 1)],
            p_send.at[d],
            p_recv.at[0],
        ).wait_send()

    for peer in ranks:
        to(
            {"dp": peer}, down_send.at[peer], down_recv.at[peer], dn_send.at[0], dn_recv.at[peer]
        ).wait_recv()
        result += down_recv[peer].astype(f32)
    for copy in dn_copies:
        copy.wait_send()
    out_ref[...] = result.astype(bf16)


def layer(
    latent_store,
    page_rank,
    page_index,
    lengths,
    queries,
    new_latent,
    up_value,
    out_proj,
    residual,
    norm_gain,
    w_gate,
    w_up,
    w_down,
):
    dp, rep = lax.axis_size("dp"), lax.axis_size("rep")
    steps, width = residual.shape
    rows = dp * steps
    hidden_width = w_gate.shape[1]
    latent_width = new_latent.shape[1]
    slots = latent_store.shape[1]
    cap = -(-slots // dp)
    half = up_value.shape[0] // CORES
    block = half * steps
    query_count = dp * block
    planes = rep // CORES
    share = query_count // planes
    vdim = up_value.shape[2]
    split = width // 2 // 256 * 256
    chunks = hidden_width // (512 if hidden_width % 512 == 0 else 128)
    dma = pltpu.SemaphoreType.DMA
    hbm = pl.BlockSpec(memory_space=pltpu.HBM)
    return pl.pallas_call(
        functools.partial(layer_kernel, dp, rep),
        out_shape=jax.ShapeDtypeStruct((steps, width), bf16),
        in_specs=[hbm] * 13,
        out_specs=pl.BlockSpec(memory_space=pltpu.VMEM),
        scratch_shapes=[
            pltpu.SMEM(page_rank.shape, i32),
            pltpu.SMEM(page_index.shape, i32),
            pltpu.SMEM(lengths.shape[::-1], i32),
            pltpu.VMEM(queries.shape, bf16),
            pltpu.VMEM(new_latent.shape, bf16),
            pltpu.VMEM(residual.shape, bf16),
            pltpu.VMEM(norm_gain.shape, f32),
            pltpu.VMEM(latent_store.shape[1:], bf16),
            pltpu.VMEM((half,) + up_value.shape[1:], bf16),
            pltpu.VMEM(out_proj.shape, bf16),
            pltpu.VMEM(w_gate.shape, bf16),
            pltpu.VMEM(w_up.shape, bf16),
            pltpu.VMEM(w_down.shape, bf16),
            pltpu.VMEM((dp, planes, share, CKV), bf16),
            pltpu.VMEM((dp, planes, share // 2, 2 * (latent_width - CKV)), bf16),
            pltpu.VMEM((dp, cap) + latent_store.shape[2:], bf16),
            pltpu.VMEM((dp, cap) + latent_store.shape[2:], bf16),
            pltpu.VMEM((dp, 8, PAGE), i32),
            pltpu.VMEM((dp, 8, PAGE), i32),
            pltpu.VMEM((dp, dp, block, CKV + PAGE), bf16),
            pltpu.VMEM((dp, dp, block, CKV + PAGE), bf16),
            pltpu.VMEM((query_count, CKV), f32),
            pltpu.VMEM((rep, rows, half * vdim), bf16),
            pltpu.VMEM((rep, rows, 128), f32),
            pltpu.VMEM((dp, rows, split), bf16),
            pltpu.VMEM((dp, rows, width - split), bf16),
            pltpu.VMEM((dp, steps, width), f32),
            pltpu.VMEM((rep, rows, 128), f32),
            pltpu.VMEM((2, rows, hidden_width), f32),
            pltpu.VMEM((rep, chunks, 2, rows, hidden_width // chunks), bf16),
            pltpu.VMEM((dp, steps, width), bf16),
            pltpu.VMEM((dp, steps, width), bf16),
            dma((13,)),
            dma((dp - 1,)),
            dma((dp,)),
            dma((dp - 1,)),
            dma((dp,)),
            dma((2, dp, planes - 1)),
            dma((2, dp, planes - 1)),
            dma((dp,)),
            dma((dp,)),
            dma((dp,)),
            dma((dp,)),
            dma((dp,)),
            dma((dp,)),
            dma((2, rep - 1)),
            dma((2, rep - 1)),
            dma((2, dp - 1)),
            dma((2, dp)),
            dma((rep - 1,)),
            dma((rep - 1,)),
            dma((chunks, rep - 1)),
            dma((chunks, rep - 1)),
            dma((dp - 1,)),
            dma((dp,)),
        ],
        compiler_params=pltpu.CompilerParams(
            collective_id=0, has_side_effects=True, vmem_limit_bytes=52 * 1024 * 1024
        ),
    )(
        *(
            pltpu.with_memory_space_constraint(item, pltpu.HBM)
            for item in (
        page_rank,
        page_index,
        lengths.T,
        queries,
        new_latent,
        residual,
        norm_gain,
        latent_store,
        up_value,
        out_proj,
        w_gate,
        w_up,
        w_down,
            )
        )
    )


def solution(mesh):
    in_specs = (
        P(("groups", "dp"), "rep", None, None),
        P("groups", "rep"),
        P("groups", "rep"),
        P("groups", None),
        P(("groups", "dp"), None),
        P(("groups", "dp"), None),
        P("dp", None, None),
        P("dp", "rep"),
        P(("groups", "dp"), "rep"),
        P("rep"),
        P("rep", "dp"),
        P("rep", "dp"),
        P("dp", "rep"),
    )
    out_specs = P(("groups", "dp"), "rep")
    return jax.shard_map(
        layer, mesh=mesh, in_specs=in_specs, out_specs=out_specs, check_vma=False
    )
```

```python
import functools
import math

import jax
import jax.numpy as jnp
from jax import lax
from jax.experimental import pallas as pl
from jax.experimental.pallas import tpu as pltpu
from jax.sharding import PartitionSpec as P

D = 7168
CKV = 512
PAGE = 128
CORES = 2

score_scale = 1.0 / math.sqrt(192.0)
epsilon = 1e-06
mask_value = -1e30
tiny = 1e-30

MESH = pl.DeviceIdType.MESH
f32, bf16, i32 = jnp.float32, jnp.bfloat16, jnp.int32


def split_three(value):
    first = value.astype(bf16)
    rest = value - first.astype(f32)
    second = rest.astype(bf16)
    third = (rest - second.astype(f32)).astype(bf16)
    return first, second, third


def layer_kernel(
    dp,
    rep,
    page_rank_hbm,
    page_index_hbm,
    lengths_hbm,
    queries_hbm,
    fresh_hbm,
    residual_hbm,
    gain_hbm,
    store_hbm,
    up_value_hbm,
    out_proj_hbm,
    w_gate_hbm,
    w_up_hbm,
    w_down_hbm,
    out_ref,
    page_rank,
    page_index,
    lengths,
    query_raw,
    fresh_raw,
    residual,
    gain,
    pages,
    up_value,
    out_proj,
    w_gate,
    w_up,
    w_down,
    queries,
    tails,
    own_pages,
    peer_pages,
    turned,
    part,
    part_recv,
    stat_sum,
    stat_part,
    stat_recv,
    latent,
    value_buf,
    level_buf,
    op_first,
    op_second,
    mixed,
    sq_buf,
    gu_sum,
    gu_buf,
    down_send,
    down_recv,
    load_sem,
    q_send,
    q_recv,
    x_send,
    x_recv,
    pg_sem,
    p_sem,
    st_sem,
    v_sem,
    op_sem,
    sq_sem,
    gu_send,
    gu_recv,
    dn_sem,
):
    my_rank = lax.axis_index("dp")
    my_column = lax.axis_index("rep")
    my_core = lax.rem(my_column, CORES)
    my_plane = my_column // CORES
    steps, width = residual.shape
    rows = dp * steps
    latent_width = fresh_raw.shape[1]
    slots = page_rank.shape[1]
    slot_total = slots * rep
    half = up_value.shape[0]
    head_group = half * CORES
    block = half * steps
    query_count = dp * block
    cap = own_pages.shape[1]
    vdim = up_value.shape[2]

    barrier = pltpu.get_barrier_semaphore()
    columns = [lax.rem(my_column + k, rep) for k in range(1, rep)]
    bits = dp.bit_length() - 1

    def flipped(mask):
        return sum((my_rank // 2**b + mask // 2**b) % 2 * 2**b for b in range(bits))

    def source(i):
        return flipped((0, 1, 3, 2)[i] if dp == 4 else i)

    ranks = [source(i) for i in range(1, dp)]
    for peer in ranks:
        pl.semaphore_signal(barrier, inc=1, device_id={"dp": peer}, device_id_type=MESH)
    for peer in columns:
        pl.semaphore_signal(barrier, inc=1, device_id={"rep": peer}, device_id_type=MESH)

    loads = []
    for i, (start, target) in enumerate(
        (
            (queries_hbm, query_raw),
            (store_hbm.at[0], pages),
            (fresh_hbm, fresh_raw),
            (residual_hbm, residual),
            (gain_hbm, gain),
            (up_value_hbm.at[pl.ds(my_core * half, half)], up_value),
            (out_proj_hbm, out_proj),
            (w_gate_hbm, w_gate),
            (w_up_hbm, w_up),
            (w_down_hbm, w_down),
            (page_rank_hbm, page_rank),
            (page_index_hbm, page_index),
            (lengths_hbm, lengths),
        )
    ):
        loads.append(pltpu.make_async_copy(start, target, load_sem.at[i]))
    for i in (0, 10, 11, 12, *range(1, 10)):
        loads[i].start()

    def to(target, start, end, send, recv):
        return pltpu.make_async_remote_copy(
            src_ref=start,
            dst_ref=end,
            send_sem=send,
            recv_sem=recv,
            device_id=target,
            device_id_type=MESH,
        )

    def send_all(axis, start, end, send, recv):
        for peer in ranks if axis == "dp" else columns:
            to({axis: peer}, start, end, send, recv).start()

    def arrived(buffer, sem):
        pltpu.make_async_copy(buffer, buffer, sem).wait()

    loads[0].wait()
    pieces = []
    for p in range(dp):
        if half * latent_width % 128 == 0:
            at = pl.ds(
                pl.multiple_of((p * head_group + my_core * half) * latent_width, 128),
                half * latent_width,
            )
            chunk = query_raw[:, at].astype(f32)
        else:
            both = query_raw[
                :, p * head_group * latent_width : (p + 1) * head_group * latent_width
            ].astype(f32)
            chunk = jnp.where(
                my_core == 0, both[:, : half * latent_width], both[:, half * latent_width :]
            )
        for s in range(steps):
            for h in range(half):
                pieces.append(chunk[s : s + 1, h * latent_width : (h + 1) * latent_width])
    planes, share = queries.shape[1:3]
    for x in range(planes):
        whole = jnp.concatenate(pieces[x * share : (x + 1) * share], axis=0)
        queries[my_rank, x] = whole[:, :CKV].astype(bf16)
        tails[my_rank, x] = jnp.concatenate(
            [whole[: share // 2, CKV:], whole[share // 2 :, CKV:]], axis=1
        ).astype(bf16)

    pl.semaphore_wait(barrier, dp - 1 + rep - 1)

    def query_copies(peer, d, near):
        return [
            to(
                {"dp": peer},
                item.at[d] if near else item.at[d, my_plane],
                item.at[d] if near else item.at[d, my_plane],
                q_send.at[2 * near + n],
                q_recv.at[n, d],
            )
            for n, item in enumerate((queries, tails))
        ]

    def plane_copies(d, arriving):
        copies = []
        for j in range(1, planes):
            peer = lax.rem(my_plane + j, planes) * CORES + my_core
            x = lax.rem(my_plane + planes - j, planes) if arriving else my_plane
            for n, item in enumerate((queries, tails)):
                copies.append(
                    to(
                        {"rep": peer},
                        item.at[d, x],
                        item.at[d, x],
                        x_send.at[n],
                        x_recv.at[n, d, j - 1],
                    )
                )
        return copies

    for j, peer in (*enumerate(ranks[1:], 1), (0, ranks[0])):
        for copy in query_copies(peer, my_rank, int(j == 0)):
            copy.start()

    partner = my_plane * CORES + (1 - my_core)
    for i in (1, 10, 11, 12):
        loads[i].wait()

    def page_copy(d):
        return to({"rep": partner}, own_pages.at[d], peer_pages.at[d], pg_sem.at[0], pg_sem.at[1 + d])

    def compact(i, carry):
        d = source(i)
        count = jnp.int32(0)
        index = [jnp.int32(0)] * cap
        limit = [jnp.int32(0)] * cap
        for q in range(slots):
            held = jnp.where(page_rank[d, q] == my_rank, 1, 0)
            place = lax.rem(my_column * slots + q, slot_total) * PAGE
            seen = jnp.clip(lengths[0, d] - place, 0, PAGE)
            for j in range(cap):
                hit = jnp.where(count == j, held, 0)
                index[j] = index[j] + hit * page_index[d, q]
                limit[j] = limit[j] + hit * seen
            count = count + held
        for j in range(cap):
            own_pages[d, j, :latent_width] = pages[index[j]]
            own_pages[d, j, latent_width:] = jnp.full(
                (own_pages.shape[2] - latent_width, PAGE), limit[j].astype(f32)
            ).astype(bf16)
        page_copy(d).start()
        return carry

    compact(0, 0)
    if dp <= 4:
        for i in range(1, dp):
            compact(i, 0)
    else:
        lax.fori_loop(1, dp, compact, 0)

    lanes = lax.broadcasted_iota(i32, (query_count, PAGE), 1)
    row_ids = lax.broadcasted_iota(i32, (query_count, PAGE), 0)

    def prepare(i, carry):
        d = source(i)
        page_copy(d).wait_recv()
        for n, pages_ref in enumerate((own_pages, peer_pages)):
            for j in range(cap):
                at = (n * cap + j) * PAGE
                turned[d, at : at + PAGE] = pages_ref[d, j, :CKV].T
        return carry

    def attend_all(group, first=False, near=False):
        ranks_here = [source(i) for i in group]
        for d in () if first else ranks_here:
            for copy in query_copies(d, d, 1) if near else plane_copies(d, True):
                copy.wait_recv()
        results = []
        for d in ranks_here:
            query = queries[d].reshape(query_count, CKV)
            tail = [tails[d, x].astype(f32) for x in range(planes)]
            tail = jnp.concatenate(
                [
                    item
                    for pair in tail
                    for item in (pair[:, : latent_width - CKV], pair[:, latent_width - CKV :])
                ],
                axis=0,
            ).astype(bf16)
            keys, visible = [], []
            for pages_ref in (own_pages, peer_pages):
                for j in range(cap):
                    keys.append(pages_ref[d, j, :latent_width])
                    limit = pages_ref[d, j, latent_width:].astype(f32)[:1]
                    visible.append(lanes < limit.astype(i32))
            keys = jnp.concatenate(keys, axis=1)
            score = (
                jnp.dot(query, keys[:CKV], preferred_element_type=f32)
                + jnp.dot(tail, keys[CKV:], preferred_element_type=f32)
            ) * score_scale
            scores = [
                jnp.where(see, score[:, n * PAGE : (n + 1) * PAGE], mask_value)
                for n, see in enumerate(visible)
            ]
            if first:
                fresh = jnp.concatenate(
                    [fresh_raw[...].astype(f32), jnp.zeros((PAGE - steps, latent_width), f32)],
                    axis=0,
                ).astype(bf16)
                across = (((1,), (1,)), ((), ()))
                extra = lax.dot_general(
                    query, fresh[:, :CKV], across, preferred_element_type=f32
                ) + lax.dot_general(tail, fresh[:, CKV:], across, preferred_element_type=f32)
                step = lax.rem(row_ids, block) // half
                see = lanes + PAGE * my_plane <= step
                visible.append(see)
                scores.append(jnp.where(see, extra * score_scale, mask_value))
            peak = jnp.max(functools.reduce(jnp.maximum, scores), axis=1, keepdims=True)
            weights = [
                jnp.where(see, jnp.exp(score - peak), 0.0)
                for see, score in zip(visible, scores, strict=True)
            ]
            total = jnp.sum(functools.reduce(jnp.add, weights), axis=1, keepdims=True)
            rounded = [weight.astype(bf16) for weight in weights]
            value = jnp.dot(
                jnp.concatenate(rounded[: CORES * cap], axis=1),
                turned[d],
                preferred_element_type=f32,
            )
            if first:
                value += jnp.dot(rounded[-1], fresh[:, :CKV], preferred_element_type=f32)
            value = value * (1.0 / jnp.maximum(total, tiny))
            level = jnp.where(
                total > 0.0, peak + jnp.log(jnp.maximum(total, tiny)), mask_value
            )
            results.append((value, level))
        for i, d, (value, level) in zip(group, ranks_here, results, strict=True):
            for p in range(dp):
                part[i, p] = value[p * block : (p + 1) * block].astype(bf16)
            for peer in ranks:
                to(
                    {"dp": peer},
                    part.at[i, peer],
                    part_recv.at[d, my_rank],
                    p_sem.at[0],
                    p_sem.at[1],
                ).start()
            part_recv[d, my_rank] = part[i, my_rank]
        stat = jnp.zeros((query_count, PAGE), f32) if first else stat_sum[...]
        for d, (value, level) in zip(ranks_here, results, strict=True):
            for n, term in enumerate(split_three(level)):
                stat = jnp.where(lanes == 3 * d + n, term.astype(f32), stat)
        stat_sum[...] = stat

    def forward(i, carry):
        d = source(i)
        for copy in query_copies(d, d, 0):
            copy.wait_recv()
        for copy in plane_copies(d, False):
            copy.start()
        return carry

    prepare(0, 0)
    loads[2].wait()
    attend_all((0,), first=True)
    if dp == 4:
        prepare(1, 0)
        for i in range(2, dp):
            forward(i, 0)
        attend_all((1,), near=True)
        for i in range(2, dp):
            prepare(i, 0)
        for i in range(2, dp):
            attend_all((i,))
    else:

        def attend(i, carry):
            attend_all((i,))
            return carry

        lax.fori_loop(2, dp, forward, 0)
        lax.fori_loop(1, dp, prepare, 0)
        attend_all((1,), near=True)
        lax.fori_loop(2, dp, attend, 0)
    for p in range(dp):
        stat_part[p] = stat_sum[p * block : (p + 1) * block].astype(bf16)
    for j, peer in enumerate(ranks):
        to(
            {"dp": peer}, stat_part.at[peer], stat_recv.at[my_rank], st_sem.at[0], st_sem.at[1]
        ).start()
    stat_recv[my_rank] = stat_part[my_rank]

    levels = []
    others = pl.ds(0, dp - 1)
    arrived(part_recv.at[others], p_sem.at[1])
    arrived(stat_recv.at[others], st_sem.at[1])
    stat = stat_recv[...].astype(f32)
    for d in range(dp):
        message = part_recv[d].astype(f32)
        level = functools.reduce(
            jnp.add, [stat[:, :, 3 * d + n : 3 * d + n + 1] for n in range(3)]
        )
        best = jnp.max(level, axis=0)
        factor = jnp.exp(level - best[None])
        total = jnp.sum(factor, axis=0)
        latent[d * block : (d + 1) * block] = (
            jnp.sum(message * (factor / total[None]), axis=0)
        )
        levels.append(best + jnp.log(total))
    loads[5].wait()
    projected = jnp.dot(
        latent[...].astype(bf16),
        jnp.concatenate([up_value[h] for h in range(half)], axis=1),
        preferred_element_type=f32,
    )
    row_head = lax.rem(lax.broadcasted_iota(i32, (query_count, 128), 0), half)
    level = jnp.where(
        row_head == lax.broadcasted_iota(i32, (query_count, 128), 1),
        jnp.concatenate(levels, axis=0),
        0.0,
    )
    picked = jnp.concatenate(
        [
            jnp.where(row_head[:, :vdim] == h, projected[:, h * vdim : (h + 1) * vdim], 0.0)
            for h in range(half)
        ],
        axis=1,
    )
    if half > 1:
        picked = jnp.sum(picked.reshape(rows, half, half * vdim), axis=1)
        level = jnp.sum(level.reshape(rows, half, 128), axis=1)
    value_buf[my_column] = picked.astype(bf16)
    level_buf[my_column] = level
    send_all("rep", value_buf.at[my_column], value_buf.at[my_column], v_sem.at[0], v_sem.at[1])
    send_all("rep", level_buf.at[my_column], level_buf.at[my_column], v_sem.at[2], v_sem.at[3])
    columns_here = pl.ds(0, rep - 1)
    for n, item in ((1, value_buf), (3, level_buf)):
        arrived(item.at[columns_here], v_sem.at[n])
    values = []
    for k in range(CORES):
        held = range(k, rep, CORES)
        best = functools.reduce(jnp.maximum, [level_buf[c] for c in held])
        factors = [jnp.exp(level_buf[c] - best) for c in held]
        total = functools.reduce(jnp.add, factors)
        factors = [factor / total for factor in factors]
        for h in range(half):
            values.append(
                functools.reduce(
                    jnp.add,
                    [
                        value_buf[c, :, h * vdim : (h + 1) * vdim].astype(f32)
                        * factor[:, h : h + 1]
                        for c, factor in zip(held, factors, strict=True)
                    ],
                )
            )
    values = jnp.concatenate(values, axis=1).astype(bf16)

    loads[3].wait()
    loads[6].wait()
    own_row = lax.broadcasted_iota(i32, (rows, 1), 0) // steps == my_rank
    kept = jnp.concatenate([residual[...].astype(f32)] * dp, axis=0)
    split = op_first.shape[2]
    spans = ((0, split, op_first), (split, width, op_second))
    parts = []
    for n, (begin, end, buffer) in enumerate(spans):
        piece = jnp.where(own_row, kept[:, begin:end], 0.0) + jnp.dot(
            values, out_proj[:, begin:end], preferred_element_type=f32
        )
        buffer[my_rank] = piece.astype(bf16)
        parts.append(piece)
        item = buffer.at[my_rank]
        send_all("dp", item, item, op_sem.at[0, n], op_sem.at[1, n])
    loads[4].wait()
    gains = gain[...].reshape(1, width)
    chunks, chunk = gu_buf.shape[1], gu_buf.shape[4]
    loads[7].wait()
    loads[8].wait()
    squares = jnp.zeros((rows, 1), f32)
    for n, (begin, end, buffer) in enumerate(spans):
        piece = parts[n]
        arrived(buffer.at[others], op_sem.at[1, n])
        for peer in ranks:
            piece += buffer[peer].astype(f32)
        for d in range(dp):
            mixed[d, :, begin:end] = piece[d * steps : (d + 1) * steps]
        squares += jnp.sum(piece * piece, axis=1, keepdims=True)
        scaled = (piece * gains[:, begin:end]).astype(bf16)
        last = n == len(spans) - 1
        if last:
            sq_buf[my_column] = jnp.broadcast_to(squares, (rows, 128))
            item = sq_buf.at[my_column]
            send_all("rep", item, item, sq_sem.at[0], sq_sem.at[1])
        for c in range(chunks):
            at = slice(c * chunk, (c + 1) * chunk)
            for m, weight in enumerate((w_gate, w_up)):
                total = jnp.dot(scaled, weight[begin:end, at], preferred_element_type=f32)
                if n > 0:
                    total += gu_sum[m, :, at]
                if last:
                    gu_buf[my_column, c, m] = total.astype(bf16)
                else:
                    gu_sum[m, :, at] = total
            if last:
                item = gu_buf.at[my_column, c]
                send_all("rep", item, item, gu_send, gu_recv.at[c])

    arrived(sq_buf.at[columns_here], sq_sem.at[1])
    total = sq_buf[0]
    for c in range(1, rep):
        total += sq_buf[c]
    scale = lax.rsqrt(total[:, :1] / D + epsilon)
    loads[9].wait()
    down = jnp.zeros((rows, width), f32)
    for c in range(chunks):
        arrived(gu_buf.at[columns_here, c], gu_recv.at[c])
        gate = gu_buf[0, c, 0].astype(f32)
        up = gu_buf[0, c, 1].astype(f32)
        for other in range(1, rep):
            gate += gu_buf[other, c, 0].astype(f32)
            up += gu_buf[other, c, 1].astype(f32)
        gate = gate * scale
        up = up * scale
        hidden = (gate / (1.0 + jnp.exp(-gate)) * up).astype(bf16)
        down += jnp.dot(
            hidden, w_down[c * chunk : (c + 1) * chunk], preferred_element_type=f32
        )
    for d in range(dp):
        down_send[d] = down[d * steps : (d + 1) * steps].astype(bf16)
    for peer in ranks:
        to(
            {"dp": peer},
            down_send.at[peer],
            down_recv.at[my_rank],
            dn_sem.at[0],
            dn_sem.at[1],
        ).start()
    result = mixed[my_rank] + down_send[my_rank].astype(f32)

    for n, item in enumerate((queries, tails)):
        arrived(item.at[pl.ds(0, dp - 2), 0], q_send.at[n])
        arrived(item.at[0], q_send.at[2 + n])
        arrived(item.at[pl.ds(0, dp - 2), pl.ds(0, planes - 1)], x_send.at[n])
    arrived(own_pages, pg_sem.at[0])
    arrived(part.at[others], p_sem.at[0])
    arrived(stat_part.at[others], st_sem.at[0])
    for n, item in ((0, value_buf), (2, level_buf)):
        arrived(item.at[columns_here], v_sem.at[n])
    for n, item in enumerate((op_first, op_second)):
        arrived(item.at[others], op_sem.at[0, n])
    arrived(sq_buf.at[columns_here], sq_sem.at[0])
    arrived(gu_buf.at[columns_here], gu_send)

    arrived(down_recv.at[others], dn_sem.at[1])
    for peer in ranks:
        result += down_recv[peer].astype(f32)
    arrived(down_send.at[others], dn_sem.at[0])
    out_ref[...] = result.astype(bf16)


def layer(
    latent_store,
    page_rank,
    page_index,
    lengths,
    queries,
    new_latent,
    up_value,
    out_proj,
    residual,
    norm_gain,
    w_gate,
    w_up,
    w_down,
):
    dp, rep = lax.axis_size("dp"), lax.axis_size("rep")
    steps, width = residual.shape
    rows = dp * steps
    hidden_width = w_gate.shape[1]
    latent_width = new_latent.shape[1]
    slots = latent_store.shape[1]
    cap = -(-slots // dp)
    half = up_value.shape[0] // CORES
    block = half * steps
    query_count = dp * block
    planes = rep // CORES
    share = query_count // planes
    vdim = up_value.shape[2]
    split = width // 2 // 256 * 256
    chunks = hidden_width // (512 if hidden_width % 512 == 0 else 128)
    dma = pltpu.SemaphoreType.DMA
    hbm = pl.BlockSpec(memory_space=pltpu.HBM)
    return pl.pallas_call(
        functools.partial(layer_kernel, dp, rep),
        out_shape=jax.ShapeDtypeStruct((steps, width), bf16),
        in_specs=[hbm] * 13,
        out_specs=pl.BlockSpec(memory_space=pltpu.VMEM),
        scratch_shapes=[
            pltpu.SMEM(page_rank.shape, i32),
            pltpu.SMEM(page_index.shape, i32),
            pltpu.SMEM(lengths.shape[::-1], i32),
            pltpu.VMEM(queries.shape, bf16),
            pltpu.VMEM(new_latent.shape, bf16),
            pltpu.VMEM(residual.shape, bf16),
            pltpu.VMEM(norm_gain.shape, f32),
            pltpu.VMEM(latent_store.shape[1:], bf16),
            pltpu.VMEM((half,) + up_value.shape[1:], bf16),
            pltpu.VMEM(out_proj.shape, bf16),
            pltpu.VMEM(w_gate.shape, bf16),
            pltpu.VMEM(w_up.shape, bf16),
            pltpu.VMEM(w_down.shape, bf16),
            pltpu.VMEM((dp, planes, share, CKV), bf16),
            pltpu.VMEM((dp, planes, share // 2, 2 * (latent_width - CKV)), bf16),
            pltpu.VMEM((dp, cap, latent_width + 16, PAGE), bf16),
            pltpu.VMEM((dp, cap, latent_width + 16, PAGE), bf16),
            pltpu.VMEM((dp, CORES * cap * PAGE, CKV), bf16),
            pltpu.VMEM((dp, dp, block, CKV), bf16),
            pltpu.VMEM((dp, dp, block, CKV), bf16),
            pltpu.VMEM((query_count, PAGE), f32),
            pltpu.VMEM((dp, block, PAGE), bf16),
            pltpu.VMEM((dp, block, PAGE), bf16),
            pltpu.VMEM((query_count, CKV), f32),
            pltpu.VMEM((rep, rows, half * vdim), bf16),
            pltpu.VMEM((rep, rows, 128), f32),
            pltpu.VMEM((dp, rows, split), bf16),
            pltpu.VMEM((dp, rows, width - split), bf16),
            pltpu.VMEM((dp, steps, width), f32),
            pltpu.VMEM((rep, rows, 128), f32),
            pltpu.VMEM((2, rows, hidden_width), f32),
            pltpu.VMEM((rep, chunks, 2, rows, hidden_width // chunks), bf16),
            pltpu.VMEM((dp, steps, width), bf16),
            pltpu.VMEM((dp, steps, width), bf16),
            dma((13,)),
            dma((4,)),
            dma((2, dp)),
            dma((2,)),
            dma((2, dp, planes - 1)),
            dma((1 + dp,)),
            dma((2,)),
            dma((2,)),
            dma((4,)),
            dma((2, 2)),
            dma((2,)),
            dma(()),
            dma((chunks,)),
            dma((2,)),
        ],
        compiler_params=pltpu.CompilerParams(
            collective_id=0, has_side_effects=True, vmem_limit_bytes=53 * 1024 * 1024
        ),
    )(
        *(
            pltpu.with_memory_space_constraint(item, pltpu.HBM)
            for item in (
        page_rank,
        page_index,
        lengths.T,
        queries,
        new_latent,
        residual,
        norm_gain,
        latent_store,
        up_value,
        out_proj,
        w_gate,
        w_up,
        w_down,
            )
        )
    )


def solution(mesh):
    in_specs = (
        P(("groups", "dp"), "rep", None, None),
        P("groups", "rep"),
        P("groups", "rep"),
        P("groups", None),
        P(("groups", "dp"), None),
        P(("groups", "dp"), None),
        P("dp", None, None),
        P("dp", "rep"),
        P(("groups", "dp"), "rep"),
        P("rep"),
        P("rep", "dp"),
        P("rep", "dp"),
        P("dp", "rep"),
    )
    out_specs = P(("groups", "dp"), "rep")
    return jax.shard_map(
        layer, mesh=mesh, in_specs=in_specs, out_specs=out_specs, check_vma=False
    )
```

```python
import functools
import math

import jax
import jax.numpy as jnp
from jax import lax
from jax.experimental import pallas as pl
from jax.experimental.pallas import tpu as pltpu
from jax.sharding import PartitionSpec as P

D = 7168
CKV = 512
PAGE = 128
CORES = 2

score_scale = 1.0 / math.sqrt(192.0)
epsilon = 1e-06
mask_value = -1e30
tiny = 1e-30

MESH = pl.DeviceIdType.MESH
f32, bf16, i32 = jnp.float32, jnp.bfloat16, jnp.int32


def split_three(value):
    first = value.astype(bf16)
    rest = value - first.astype(f32)
    second = rest.astype(bf16)
    third = (rest - second.astype(f32)).astype(bf16)
    return first, second, third


def layer_kernel(
    dp,
    rep,
    page_rank_hbm,
    page_index_hbm,
    lengths_hbm,
    queries_hbm,
    fresh_hbm,
    residual_hbm,
    gain_hbm,
    store_hbm,
    up_value_hbm,
    out_proj_hbm,
    w_gate_hbm,
    w_up_hbm,
    w_down_hbm,
    out_ref,
    page_rank,
    page_index,
    lengths,
    query_raw,
    fresh_raw,
    residual,
    gain,
    pages,
    up_value,
    out_proj,
    w_gate,
    w_up,
    w_down,
    queries,
    tails,
    own_pages,
    peer_pages,
    turned,
    part,
    part_recv,
    stat_sum,
    stat_part,
    stat_recv,
    latent,
    value_buf,
    level_buf,
    op_first,
    op_second,
    mixed,
    sq_buf,
    gu_sum,
    gu_buf,
    down_send,
    down_recv,
    load_sem,
    q_send,
    q_recv,
    x_send,
    x_recv,
    pg_sem,
    p_sem,
    st_sem,
    v_sem,
    op_sem,
    sq_sem,
    gu_send,
    gu_recv,
    dn_sem,
):
    my_rank = lax.axis_index("dp")
    my_column = lax.axis_index("rep")
    my_core = lax.rem(my_column, CORES)
    my_plane = my_column // CORES
    steps, width = residual.shape
    rows = dp * steps
    latent_width = fresh_raw.shape[1]
    slots = page_rank.shape[1]
    slot_total = slots * rep
    half = up_value.shape[0]
    head_group = half * CORES
    block = half * steps
    query_count = dp * block
    cap = own_pages.shape[1]
    vdim = up_value.shape[2]

    barrier = pltpu.get_barrier_semaphore()
    columns = [
        lax.rem(my_plane + j, rep // CORES) * CORES + core
        for j in (*range(1, rep // CORES), 0)
        for core in ((my_core, 1 - my_core) if j else (1 - my_core,))
    ]
    bits = dp.bit_length() - 1

    def flipped(mask):
        return sum((my_rank // 2**b + mask // 2**b) % 2 * 2**b for b in range(bits))

    def source(i):
        return flipped((0, 1, 3, 2)[i] if dp == 4 else i)

    ranks = [source(i) for i in range(1, dp)]
    for peer in ranks:
        pl.semaphore_signal(barrier, inc=1, device_id={"dp": peer}, device_id_type=MESH)
    for peer in columns:
        pl.semaphore_signal(barrier, inc=1, device_id={"rep": peer}, device_id_type=MESH)

    loads = []
    for i, (start, target) in enumerate(
        (
            (queries_hbm, query_raw),
            (store_hbm.at[0], pages),
            (fresh_hbm, fresh_raw),
            (residual_hbm, residual),
            (gain_hbm, gain),
            (up_value_hbm.at[pl.ds(my_core * half, half)], up_value),
            (out_proj_hbm, out_proj),
            (w_gate_hbm, w_gate),
            (w_up_hbm, w_up),
            (w_down_hbm, w_down),
            (page_rank_hbm, page_rank),
            (page_index_hbm, page_index),
            (lengths_hbm, lengths),
        )
    ):
        loads.append(pltpu.make_async_copy(start, target, load_sem.at[i]))
    for i in (0, 10, 11, 12, *range(1, 10)):
        loads[i].start()

    def to(target, start, end, send, recv):
        return pltpu.make_async_remote_copy(
            src_ref=start,
            dst_ref=end,
            send_sem=send,
            recv_sem=recv,
            device_id=target,
            device_id_type=MESH,
        )

    def send_all(axis, start, end, send, recv):
        for peer in ranks if axis == "dp" else columns:
            to({axis: peer}, start, end, send, recv).start()

    def arrived(buffer, sem):
        pltpu.make_async_copy(buffer, buffer, sem).wait()

    loads[0].wait()
    pieces = []
    for p in range(dp):
        if half * latent_width % 128 == 0:
            at = pl.ds(
                pl.multiple_of((p * head_group + my_core * half) * latent_width, 128),
                half * latent_width,
            )
            chunk = query_raw[:, at].astype(f32)
        else:
            both = query_raw[
                :, p * head_group * latent_width : (p + 1) * head_group * latent_width
            ].astype(f32)
            chunk = jnp.where(
                my_core == 0, both[:, : half * latent_width], both[:, half * latent_width :]
            )
        for s in range(steps):
            for h in range(half):
                pieces.append(chunk[s : s + 1, h * latent_width : (h + 1) * latent_width])
    planes, share = queries.shape[1:3]
    for x in range(planes):
        whole = jnp.concatenate(pieces[x * share : (x + 1) * share], axis=0)
        queries[my_rank, x] = whole[:, :CKV].astype(bf16)
        tails[my_rank, x] = jnp.concatenate(
            [whole[: share // 2, CKV:], whole[share // 2 :, CKV:]], axis=1
        ).astype(bf16)

    pl.semaphore_wait(barrier, dp - 1 + rep - 1)

    def query_copies(peer, d, near):
        return [
            to(
                {"dp": peer},
                item.at[d] if near else item.at[d, my_plane],
                item.at[d] if near else item.at[d, my_plane],
                q_send.at[2 * near + n],
                q_recv.at[n, d],
            )
            for n, item in enumerate((queries, tails))
        ]

    def plane_copies(d, arriving):
        copies = []
        for j in range(1, planes):
            peer = lax.rem(my_plane + j, planes) * CORES + my_core
            x = lax.rem(my_plane + planes - j, planes) if arriving else my_plane
            for n, item in enumerate((queries, tails)):
                copies.append(
                    to(
                        {"rep": peer},
                        item.at[d, x],
                        item.at[d, x],
                        x_send.at[n],
                        x_recv.at[n, d, j - 1],
                    )
                )
        return copies

    for j, peer in (*enumerate(ranks[1:], 1), (0, ranks[0])):
        for copy in query_copies(peer, my_rank, int(j == 0)):
            copy.start()

    partner = my_plane * CORES + (1 - my_core)
    for i in (1, 10, 11, 12):
        loads[i].wait()

    def page_copy(d):
        return to({"rep": partner}, own_pages.at[d], peer_pages.at[d], pg_sem.at[0], pg_sem.at[1 + d])

    def compact(i, carry):
        d = source(i)
        count = jnp.int32(0)
        index = [jnp.int32(0)] * cap
        limit = [jnp.int32(0)] * cap
        for q in range(slots):
            held = jnp.where(page_rank[d, q] == my_rank, 1, 0)
            place = lax.rem(my_column * slots + q, slot_total) * PAGE
            seen = jnp.clip(lengths[0, d] - place, 0, PAGE)
            for j in range(cap):
                hit = jnp.where(count == j, held, 0)
                index[j] = index[j] + hit * page_index[d, q]
                limit[j] = limit[j] + hit * seen
            count = count + held
        for j in range(cap):
            own_pages[d, j, :latent_width] = pages[index[j]]
            own_pages[d, j, latent_width:] = jnp.full(
                (own_pages.shape[2] - latent_width, PAGE), limit[j].astype(f32)
            ).astype(bf16)
        page_copy(d).start()
        return carry

    compact(0, 0)
    if dp <= 4:
        for i in range(1, dp):
            compact(i, 0)
    else:
        lax.fori_loop(1, dp, compact, 0)

    lanes = lax.broadcasted_iota(i32, (query_count, PAGE), 1)
    row_ids = lax.broadcasted_iota(i32, (query_count, PAGE), 0)

    def prepare(i, carry):
        d = source(i)
        page_copy(d).wait_recv()
        for n, pages_ref in enumerate((own_pages, peer_pages)):
            for j in range(cap):
                at = (n * cap + j) * PAGE
                turned[d, at : at + PAGE] = pages_ref[d, j, :CKV].T
        return carry

    def attend(group, first=False, waits=(), x=None, last=True):
        members = [source(i) for i in group]
        for copy in waits:
            copy.wait_recv()
        count = query_count if x is None else share
        across = (((1,), (1,)), ((), ()))
        if first:
            fresh = jnp.concatenate(
                [fresh_raw[...].astype(f32), jnp.zeros((PAGE - steps, latent_width), f32)],
                axis=0,
            ).astype(bf16)
        raw = []
        for d in members:
            if x is None:
                query = queries[d].reshape(query_count, CKV)
                tail = [tails[d, y].astype(f32) for y in range(planes)]
            else:
                query = queries[d, x]
                tail = [tails[d, x].astype(f32)]
            tail = jnp.concatenate(
                [
                    item
                    for pair in tail
                    for item in (pair[:, : latent_width - CKV], pair[:, latent_width - CKV :])
                ],
                axis=0,
            ).astype(bf16)
            keys = jnp.concatenate(
                [ref[d, j, :latent_width] for ref in (own_pages, peer_pages) for j in range(cap)],
                axis=1,
            )
            score = jnp.dot(query, keys[:CKV], preferred_element_type=f32) + jnp.dot(
                tail, keys[CKV:], preferred_element_type=f32
            )
            if first:
                extra = lax.dot_general(
                    query, fresh[:, :CKV], across, preferred_element_type=f32
                ) + lax.dot_general(tail, fresh[:, CKV:], across, preferred_element_type=f32)
                score = jnp.concatenate([score, extra], axis=1)
            raw.append(score)
        weighed = []
        for d, score in zip(members, raw, strict=True):
            visible = []
            for ref in (own_pages, peer_pages):
                for j in range(cap):
                    limit = ref[d, j, latent_width:].astype(f32)[:1]
                    visible.append(lanes[:count] < limit.astype(i32))
            if first:
                step = lax.rem(row_ids, block) // half
                visible.append(lanes + PAGE * my_plane <= step)
            scores = [
                jnp.where(see, score[:, n * PAGE : (n + 1) * PAGE] * score_scale, mask_value)
                for n, see in enumerate(visible)
            ]
            peak = jnp.max(functools.reduce(jnp.maximum, scores), axis=1, keepdims=True)
            weights = [
                jnp.where(see, jnp.exp(score - peak), 0.0)
                for see, score in zip(visible, scores, strict=True)
            ]
            total = jnp.sum(functools.reduce(jnp.add, weights), axis=1, keepdims=True)
            weighed.append((peak, total, [weight.astype(bf16) for weight in weights]))
        outcome = []
        for d, (peak, total, rounded) in zip(members, weighed, strict=True):
            value = jnp.dot(
                jnp.concatenate(rounded[: CORES * cap], axis=1),
                turned[d],
                preferred_element_type=f32,
            )
            if first:
                value += jnp.dot(rounded[-1], fresh[:, :CKV], preferred_element_type=f32)
            outcome.append(value * (1.0 / jnp.maximum(total, tiny)))

        def send_part(i, d, p):
            to(
                {"dp": p},
                part.at[i, p],
                part_recv.at[d, my_rank],
                p_sem.at[0],
                p_sem.at[1],
            ).start()

        for i, d, value in zip(group, members, outcome, strict=True):
            if x is None:
                for p in range(dp):
                    part[i, p] = value[p * block : (p + 1) * block].astype(bf16)
                for peer in ranks:
                    send_part(i, d, peer)
            else:
                for q in range(dp // planes):
                    p = x * (dp // planes) + q
                    part[i, p] = value[q * block : (q + 1) * block].astype(bf16)
                    pl.when(p != my_rank)(functools.partial(send_part, i, d, p))
            if last:
                part_recv[d, my_rank] = part[i, my_rank]
        terms = []
        for peak, total, rounded in weighed:
            level = jnp.where(total > 0.0, peak + jnp.log(jnp.maximum(total, tiny)), mask_value)
            terms.append([term.astype(f32) for term in split_three(level)])
        for y in range(planes) if x is None else (x,):
            at = y * share if x is None else 0
            stat = jnp.zeros((share, PAGE), f32) if first else stat_sum[y]
            for d, items in zip(members, terms, strict=True):
                for n, term in enumerate(items):
                    stat = jnp.where(lanes[:share] == 3 * d + n, term[at : at + share], stat)
            stat_sum[y] = stat

    def forward(i, carry):
        d = source(i)
        for copy in query_copies(d, d, 0):
            copy.wait_recv()
        for copy in plane_copies(d, False):
            copy.start()
        return carry

    prepare(0, 0)
    loads[2].wait()
    attend((0,), first=True)
    near_waits = query_copies(ranks[0], ranks[0], 1)
    if dp == 4:
        prepare(1, 0)
        for i in range(2, dp):
            forward(i, 0)
        attend((1,), waits=near_waits)
        for i in range(2, dp):
            prepare(i, 0)
        attend((2, 3), x=my_plane, last=False)
        for j in range(1, planes):
            attend(
                (2, 3),
                waits=[copy for i in (2, 3) for copy in plane_copies(source(i), True)]
                if j == 1
                else (),
                x=lax.rem(my_plane + planes - j, planes),
                last=j == planes - 1,
            )
    else:

        def attend_other(i, carry):
            attend((i,), waits=plane_copies(source(i), True))
            return carry

        lax.fori_loop(2, dp, forward, 0)
        lax.fori_loop(1, dp, prepare, 0)
        attend((1,), waits=near_waits)
        lax.fori_loop(2, dp, attend_other, 0)
    for p in range(dp):
        x, at = divmod(p * block, share)
        stat_part[p] = stat_sum[x, at : at + block].astype(bf16)
    for j, peer in enumerate(ranks):
        to(
            {"dp": peer}, stat_part.at[peer], stat_recv.at[my_rank], st_sem.at[0], st_sem.at[1]
        ).start()
    stat_recv[my_rank] = stat_part[my_rank]

    levels = []
    others = pl.ds(0, dp - 1)
    arrived(part_recv.at[others], p_sem.at[1])
    arrived(stat_recv.at[others], st_sem.at[1])
    stat = stat_recv[...].astype(f32)
    for d in range(dp):
        message = part_recv[d].astype(f32)
        level = functools.reduce(
            jnp.add, [stat[:, :, 3 * d + n : 3 * d + n + 1] for n in range(3)]
        )
        best = jnp.max(level, axis=0)
        factor = jnp.exp(level - best[None])
        total = jnp.sum(factor, axis=0)
        latent[d * block : (d + 1) * block] = (
            jnp.sum(message * (factor / total[None]), axis=0)
        )
        levels.append(best + jnp.log(total))
    loads[5].wait()
    projected = jnp.dot(
        latent[...].astype(bf16),
        jnp.concatenate([up_value[h] for h in range(half)], axis=1),
        preferred_element_type=f32,
    )
    row_head = lax.rem(lax.broadcasted_iota(i32, (query_count, 128), 0), half)
    level = jnp.where(
        row_head == lax.broadcasted_iota(i32, (query_count, 128), 1),
        jnp.concatenate(levels, axis=0),
        0.0,
    )
    picked = jnp.concatenate(
        [
            jnp.where(row_head[:, :vdim] == h, projected[:, h * vdim : (h + 1) * vdim], 0.0)
            for h in range(half)
        ],
        axis=1,
    )
    if half > 1:
        picked = jnp.sum(picked.reshape(rows, half, half * vdim), axis=1)
        level = jnp.sum(level.reshape(rows, half, 128), axis=1)
    value_buf[my_column] = picked.astype(bf16)
    level_buf[my_column] = level
    send_all("rep", value_buf.at[my_column], value_buf.at[my_column], v_sem.at[0], v_sem.at[1])
    send_all("rep", level_buf.at[my_column], level_buf.at[my_column], v_sem.at[2], v_sem.at[3])
    columns_here = pl.ds(0, rep - 1)
    for n, item in ((1, value_buf), (3, level_buf)):
        arrived(item.at[columns_here], v_sem.at[n])
    values = []
    for k in range(CORES):
        held = range(k, rep, CORES)
        best = functools.reduce(jnp.maximum, [level_buf[c] for c in held])
        factors = [jnp.exp(level_buf[c] - best) for c in held]
        total = functools.reduce(jnp.add, factors)
        factors = [factor / total for factor in factors]
        for h in range(half):
            values.append(
                functools.reduce(
                    jnp.add,
                    [
                        value_buf[c, :, h * vdim : (h + 1) * vdim].astype(f32)
                        * factor[:, h : h + 1]
                        for c, factor in zip(held, factors, strict=True)
                    ],
                )
            )
    values = jnp.concatenate(values, axis=1).astype(bf16)

    loads[3].wait()
    loads[6].wait()
    own_row = lax.broadcasted_iota(i32, (rows, 1), 0) // steps == my_rank
    kept = jnp.concatenate([residual[...].astype(f32)] * dp, axis=0)
    split = op_first.shape[2]
    spans = ((0, split, op_first), (split, width, op_second))
    parts = []
    for n, (begin, end, buffer) in enumerate(spans):
        piece = jnp.where(own_row, kept[:, begin:end], 0.0) + jnp.dot(
            values, out_proj[:, begin:end], preferred_element_type=f32
        )
        buffer[my_rank] = piece.astype(bf16)
        parts.append(piece)
        item = buffer.at[my_rank]
        send_all("dp", item, item, op_sem.at[0, n], op_sem.at[1, n])
    loads[4].wait()
    gains = gain[...].reshape(1, width)
    chunks, chunk = gu_buf.shape[1], gu_buf.shape[4]
    loads[7].wait()
    loads[8].wait()
    squares = jnp.zeros((rows, 1), f32)
    for n, (begin, end, buffer) in enumerate(spans):
        piece = parts[n]
        arrived(buffer.at[others], op_sem.at[1, n])
        for peer in ranks:
            piece += buffer[peer].astype(f32)
        for d in range(dp):
            mixed[d, :, begin:end] = piece[d * steps : (d + 1) * steps]
        squares += jnp.sum(piece * piece, axis=1, keepdims=True)
        scaled = (piece * gains[:, begin:end]).astype(bf16)
        last = n == len(spans) - 1
        if last:
            sq_buf[my_column] = jnp.broadcast_to(squares, (rows, 128))
            item = sq_buf.at[my_column]
            send_all("rep", item, item, sq_sem.at[0], sq_sem.at[1])
        for c in range(chunks):
            at = slice(c * chunk, (c + 1) * chunk)
            for m, weight in enumerate((w_gate, w_up)):
                total = jnp.dot(scaled, weight[begin:end, at], preferred_element_type=f32)
                if n > 0:
                    total += gu_sum[m, :, at]
                if last:
                    gu_buf[my_column, c, m] = total.astype(bf16)
                else:
                    gu_sum[m, :, at] = total
            if last:
                item = gu_buf.at[my_column, c]
                send_all("rep", item, item, gu_send, gu_recv.at[c])

    arrived(sq_buf.at[columns_here], sq_sem.at[1])
    total = sq_buf[0]
    for c in range(1, rep):
        total += sq_buf[c]
    scale = lax.rsqrt(total[:, :1] / D + epsilon)
    loads[9].wait()
    down = jnp.zeros((rows, width), f32)
    for c in range(chunks):
        arrived(gu_buf.at[columns_here, c], gu_recv.at[c])
        gate = gu_buf[0, c, 0].astype(f32)
        up = gu_buf[0, c, 1].astype(f32)
        for other in range(1, rep):
            gate += gu_buf[other, c, 0].astype(f32)
            up += gu_buf[other, c, 1].astype(f32)
        gate = gate * scale
        up = up * scale
        hidden = (gate / (1.0 + jnp.exp(-gate)) * up).astype(bf16)
        down += jnp.dot(
            hidden, w_down[c * chunk : (c + 1) * chunk], preferred_element_type=f32
        )
    for d in range(dp):
        down_send[d] = down[d * steps : (d + 1) * steps].astype(bf16)
    for peer in ranks:
        to(
            {"dp": peer},
            down_send.at[peer],
            down_recv.at[my_rank],
            dn_sem.at[0],
            dn_sem.at[1],
        ).start()
    result = mixed[my_rank] + down_send[my_rank].astype(f32)

    for n, item in enumerate((queries, tails)):
        arrived(item.at[pl.ds(0, dp - 2), 0], q_send.at[n])
        arrived(item.at[0], q_send.at[2 + n])
        arrived(item.at[pl.ds(0, dp - 2), pl.ds(0, planes - 1)], x_send.at[n])
    arrived(own_pages, pg_sem.at[0])
    arrived(part.at[others], p_sem.at[0])
    arrived(stat_part.at[others], st_sem.at[0])
    for n, item in ((0, value_buf), (2, level_buf)):
        arrived(item.at[columns_here], v_sem.at[n])
    for n, item in enumerate((op_first, op_second)):
        arrived(item.at[others], op_sem.at[0, n])
    arrived(sq_buf.at[columns_here], sq_sem.at[0])
    arrived(gu_buf.at[columns_here], gu_send)

    arrived(down_recv.at[others], dn_sem.at[1])
    for peer in ranks:
        result += down_recv[peer].astype(f32)
    arrived(down_send.at[others], dn_sem.at[0])
    out_ref[...] = result.astype(bf16)


def layer(
    latent_store,
    page_rank,
    page_index,
    lengths,
    queries,
    new_latent,
    up_value,
    out_proj,
    residual,
    norm_gain,
    w_gate,
    w_up,
    w_down,
):
    dp, rep = lax.axis_size("dp"), lax.axis_size("rep")
    steps, width = residual.shape
    rows = dp * steps
    hidden_width = w_gate.shape[1]
    latent_width = new_latent.shape[1]
    slots = latent_store.shape[1]
    cap = -(-slots // dp)
    half = up_value.shape[0] // CORES
    block = half * steps
    query_count = dp * block
    planes = rep // CORES
    share = query_count // planes
    vdim = up_value.shape[2]
    split = width // 3 // 256 * 256
    chunks = hidden_width // (512 if hidden_width % 512 == 0 else 128)
    dma = pltpu.SemaphoreType.DMA
    hbm = pl.BlockSpec(memory_space=pltpu.HBM)
    return pl.pallas_call(
        functools.partial(layer_kernel, dp, rep),
        out_shape=jax.ShapeDtypeStruct((steps, width), bf16),
        in_specs=[hbm] * 13,
        out_specs=pl.BlockSpec(memory_space=pltpu.VMEM),
        scratch_shapes=[
            pltpu.SMEM(page_rank.shape, i32),
            pltpu.SMEM(page_index.shape, i32),
            pltpu.SMEM(lengths.shape[::-1], i32),
            pltpu.VMEM(queries.shape, bf16),
            pltpu.VMEM(new_latent.shape, bf16),
            pltpu.VMEM(residual.shape, bf16),
            pltpu.VMEM(norm_gain.shape, f32),
            pltpu.VMEM(latent_store.shape[1:], bf16),
            pltpu.VMEM((half,) + up_value.shape[1:], bf16),
            pltpu.VMEM(out_proj.shape, bf16),
            pltpu.VMEM(w_gate.shape, bf16),
            pltpu.VMEM(w_up.shape, bf16),
            pltpu.VMEM(w_down.shape, bf16),
            pltpu.VMEM((dp, planes, share, CKV), bf16),
            pltpu.VMEM((dp, planes, share // 2, 2 * (latent_width - CKV)), bf16),
            pltpu.VMEM((dp, cap, latent_width + 16, PAGE), bf16),
            pltpu.VMEM((dp, cap, latent_width + 16, PAGE), bf16),
            pltpu.VMEM((dp, CORES * cap * PAGE, CKV), bf16),
            pltpu.VMEM((dp, dp, block, CKV), bf16),
            pltpu.VMEM((dp, dp, block, CKV), bf16),
            pltpu.VMEM((planes, share, PAGE), f32),
            pltpu.VMEM((dp, block, PAGE), bf16),
            pltpu.VMEM((dp, block, PAGE), bf16),
            pltpu.VMEM((query_count, CKV), f32),
            pltpu.VMEM((rep, rows, half * vdim), bf16),
            pltpu.VMEM((rep, rows, 128), f32),
            pltpu.VMEM((dp, rows, split), bf16),
            pltpu.VMEM((dp, rows, width - split), bf16),
            pltpu.VMEM((dp, steps, width), f32),
            pltpu.VMEM((rep, rows, 128), f32),
            pltpu.VMEM((2, rows, hidden_width), f32),
            pltpu.VMEM((rep, chunks, 2, rows, hidden_width // chunks), bf16),
            pltpu.VMEM((dp, steps, width), bf16),
            pltpu.VMEM((dp, steps, width), bf16),
            dma((13,)),
            dma((4,)),
            dma((2, dp)),
            dma((2,)),
            dma((2, dp, planes - 1)),
            dma((1 + dp,)),
            dma((2,)),
            dma((2,)),
            dma((4,)),
            dma((2, 2)),
            dma((2,)),
            dma(()),
            dma((chunks,)),
            dma((2,)),
        ],
        compiler_params=pltpu.CompilerParams(
            collective_id=0, has_side_effects=True, vmem_limit_bytes=53 * 1024 * 1024
        ),
    )(
        *(
            pltpu.with_memory_space_constraint(item, pltpu.HBM)
            for item in (
        page_rank,
        page_index,
        lengths.T,
        queries,
        new_latent,
        residual,
        norm_gain,
        latent_store,
        up_value,
        out_proj,
        w_gate,
        w_up,
        w_down,
            )
        )
    )


def solution(mesh):
    in_specs = (
        P(("groups", "dp"), "rep", None, None),
        P("groups", "rep"),
        P("groups", "rep"),
        P("groups", None),
        P(("groups", "dp"), None),
        P(("groups", "dp"), None),
        P("dp", None, None),
        P("dp", "rep"),
        P(("groups", "dp"), "rep"),
        P("rep"),
        P("rep", "dp"),
        P("rep", "dp"),
        P("dp", "rep"),
    )
    out_specs = P(("groups", "dp"), "rep")
    return jax.shard_map(
        layer, mesh=mesh, in_specs=in_specs, out_specs=out_specs, check_vma=False
    )
```
